32 devices in a mesh: sys: 2 (over x), aux: 4 (over z), orb: 4 (over y, core).
Axes of the slice: x: 2, y: 2, z: 4, core: 2. Of those that a mesh axis runs over, the one named last changes fastest.
Arguments:
- aux_ints: float32 [1792, 320, 320], P(('sys', 'aux'), 'orb'), parts along dimension 0
- metric: float32 [1792, 896], P(('sys', 'aux')), parts along dimension 0
- orbitals: float32 [2, 320, 32], P('sys'), parts along dimension 0
Outputs:
- output: float32 [2, 320, 320], P('sys', 'orb', 'aux'), parts along dimension 0
There are 2 independent parts. The reference program is written for one: setup_inputs(seed, part) draws one part's arguments, and reference() takes and returns one part's arrays. A program takes and returns all parts, laid end to end along the dimension named above; each array names one.
All inputs are finite; a program needn't handle non-finite values.
Results may differ from the reference program's by a relative error of at most 0.001.
Values are sent between devices in bfloat16 or wider.
A program may use at most 1 GiB of HBM per device.

```python
import jax
import jax.numpy as jnp
from jax import lax

N_AUX = 896
N_BASIS = 320
N_OCC = 32
DENS = 1

PRECISE = lax.Precision.HIGHEST


def setup_inputs(seed: int = 0, part: int = 0) -> dict:
    base_key = jax.random.fold_in(jax.random.key(seed), part)
    sub_keys = jax.random.split(base_key, 6)
    rank_b = 4
    rank_m = 4
    coh_scale = (2.0 * N_AUX * N_OCC) ** -0.5 * rank_b ** -0.25
    noise_scale = 2.0 * coh_scale
    coeffs = jax.random.normal(sub_keys[0], (N_AUX, rank_b), jnp.float32)
    patterns = jax.random.normal(sub_keys[1], (rank_b, N_BASIS), jnp.float32)
    row_keys = jax.random.split(sub_keys[2], N_AUX)

    def one_row(row_args):
        row_key, coeff_row = row_args
        noise_mat = jax.random.normal(row_key, (N_BASIS, N_BASIS), jnp.float32)
        sym_noise = (noise_mat + noise_mat.T) * (0.5 ** 0.5)
        low_rank = jnp.einsum('k,km,kl->ml', coeff_row, patterns, patterns)
        return noise_scale * sym_noise + coh_scale * low_rank

    aux_ints = lax.map(one_row, (row_keys, coeffs))
    spread = jax.random.normal(sub_keys[3], (N_AUX, N_AUX), jnp.float32)
    sym_spread = (spread + spread.T) * (0.125 / N_AUX) ** 0.5
    directions = jax.random.normal(sub_keys[4], (rank_m, N_AUX), jnp.float32) * N_AUX ** -0.5
    boost_scale = (N_AUX / rank_m) ** 0.5
    metric = jnp.eye(N_AUX, dtype=jnp.float32) + sym_spread + boost_scale * jnp.dot(directions.T, directions)
    orbitals = jax.random.normal(sub_keys[5], (DENS, N_BASIS, N_OCC), jnp.float32) * N_BASIS ** -0.5
    return {'aux_ints': aux_ints, 'metric': metric, 'orbitals': orbitals}


def reference(aux_ints, metric, orbitals):
    def one_density(coeff_mat):
        half_tr = jnp.einsum('qml,li->qmi', aux_ints, coeff_mat, precision=PRECISE)
        fitted = jnp.einsum('pq,qmi->pmi', metric, half_tr, precision=PRECISE)
        exchange = jnp.einsum('pmi,pni->mn', fitted, fitted, precision=PRECISE)
        gamma_raw = jnp.einsum('qmi,mi->q', half_tr, coeff_mat, precision=PRECISE)
        gamma_fit = jnp.dot(metric, gamma_raw, precision=PRECISE)
        weights = jnp.dot(gamma_fit, metric, precision=PRECISE)
        coulomb = jnp.einsum('q,qmn->mn', weights, aux_ints, precision=PRECISE)
        return 2.0 * coulomb - exchange

    return lax.map(one_density, orbitals)
```

```python
import jax
import jax.numpy as jnp
from jax import lax
from jax.sharding import PartitionSpec as P

PRECISE = lax.Precision.HIGHEST


def solution(mesh):
    n_aux, n_orb = mesh.shape['aux'], mesh.shape['orb']
    n_dev = n_aux * n_orb

    def local_fock(ints_blk, metric_blk, orbitals):
        q_loc, m_loc, n_bas = ints_blk.shape
        occ = orbitals.shape[2]
        coeff = orbitals[0]
        metric_all = lax.all_gather(metric_blk.astype(jnp.bfloat16), 'aux', axis=0, tiled=True)
        row_start = lax.axis_index('orb') * m_loc
        half_tr = jnp.einsum('qml,li->qmi', ints_blk, coeff, precision=PRECISE, preferred_element_type=jnp.float32)
        orb_rows = lax.dynamic_slice_in_dim(coeff, row_start, m_loc, axis=0)
        gamma_part = jnp.sum(half_tr * orb_rows[None], axis=(1, 2))[None]
        packed = jnp.transpose(half_tr, (2, 1, 0)).astype(jnp.bfloat16).reshape(n_dev, occ // n_dev, m_loc, q_loc)
        moved = lax.all_to_all(packed, ('aux', 'orb'), split_axis=0, concat_axis=0, tiled=True)
        gamma_raw = lax.psum(gamma_part, 'orb')
        gamma_all = lax.all_gather(gamma_raw, 'aux', axis=1, tiled=True)
        gamma_fit = jnp.einsum('dq,pq->dp', gamma_all, metric_blk, precision=PRECISE, preferred_element_type=jnp.float32)
        weight_part = jnp.dot(gamma_fit, metric_blk, precision=PRECISE, preferred_element_type=jnp.float32)
        weights = lax.psum_scatter(weight_part, 'aux', scatter_dimension=1, tiled=True)
        coulomb = jnp.einsum('dq,qmn->mn', weights, ints_blk, precision=PRECISE, preferred_element_type=jnp.float32)
        moved = moved.reshape(n_aux, n_orb, occ // n_dev, m_loc, q_loc)
        fitted = jnp.einsum('aoimq,aqp->iomp', moved.astype(jnp.float32),
                            metric_all.astype(jnp.float32).reshape(n_aux, q_loc, -1),
                            precision=PRECISE, preferred_element_type=jnp.float32)
        fitted = fitted.reshape(occ // n_dev, n_orb * m_loc, -1)
        exchange = jnp.einsum('imp,inp->mn', fitted, fitted, precision=PRECISE, preferred_element_type=jnp.float32)
        fock = lax.dynamic_update_slice_in_dim(
            -exchange, lax.dynamic_slice_in_dim(-exchange, row_start, m_loc, axis=0) + 2.0 * coulomb, row_start, axis=0)
        fock = lax.psum_scatter(fock, 'orb', scatter_dimension=0, tiled=True)
        return lax.psum_scatter(fock, 'aux', scatter_dimension=1, tiled=True)[None]

    return jax.shard_map(local_fock, mesh=mesh, in_specs=(P(('sys', 'aux'), 'orb', None), P(('sys', 'aux'), None), P('sys', None, None)), out_specs=P('sys', 'orb', 'aux'), check_vma=False)
```

```python
import functools

import jax
import jax.numpy as jnp
from jax import lax
from jax.experimental import pallas as pl
from jax.experimental.pallas import tpu as pltpu
from jax.sharding import PartitionSpec as P

F32, BF16 = jnp.float32, jnp.bfloat16
MESH = pl.DeviceIdType.MESH
NT = (((1,), (1,)), ((), ()))
AHEAD = 3
SLOTS = 4


def split3(x):
    h0 = x.astype(BF16)
    r1 = x - h0.astype(F32)
    h1 = r1.astype(BF16)
    r2 = r1 - h1.astype(F32)
    return h0, h1, r2.astype(BF16)


def dot(a, b):
    return jnp.dot(a, b, preferred_element_type=F32)


def dot_nt(a, b):
    return lax.dot_general(a, b, NT, preferred_element_type=F32)


def kernel(b_hbm, m_hbm, c_ref, out_ref, bb, b3, stage, sbuf, rbuf, mall, mown, cb, c3, tt, ks, jacc, gam, gsend, grecv,
           fsend, frecv, wb, gs, gr, b_sem, m_sem, s_send, s_recv, mz_send, mz_recv, mf_send, mf_recv, g_send, g_recv,
           f_send, f_recv, r_send, r_recv):
    a, o = lax.axis_index('aux'), lax.axis_index('orb')
    me = a * 4 + o
    planes = [(a + 2) % 4, 3 - a, a + 1 - 2 * (a % 2), a]
    peers = [(planes[k // 4], (o + k % 4) % 4) for k in range(16) if k != 12]

    def remote(src, dst, send, recv, dest):
        return pltpu.make_async_remote_copy(src_ref=src, dst_ref=dst, send_sem=send, recv_sem=recv,
                                            device_id={'aux': dest[0], 'orb': dest[1]}, device_id_type=MESH)

    def b_copies(g):
        slot = lax.rem(g, SLOTS)
        rows = pl.ds(pl.multiple_of(g * 8, 8), 8)
        return [pltpu.make_async_copy(b_hbm.at[:, rows, pl.ds(0, 128)], bb.at[0, g], b_sem.at[0, slot]),
                pltpu.make_async_copy(b_hbm.at[:, rows, pl.ds(128, 128)], bb.at[1, g], b_sem.at[1, slot]),
                pltpu.make_async_copy(b_hbm.at[:, rows, pl.ds(256, 64)], b3.at[slot], b_sem.at[2, slot])]

    for g in range(AHEAD):
        for cp in b_copies(g):
            cp.start()
    m_copy = pltpu.make_async_copy(m_hbm, mown, m_sem)
    m_copy.start()

    barrier = pltpu.get_barrier_semaphore()
    for dest in peers:
        pl.semaphore_signal(barrier, inc=1, device_id={'aux': dest[0], 'orb': dest[1]}, device_id_type=MESH)

    ct = jnp.transpose(c_ref[...])
    parts = split3(ct)
    zero64 = jnp.zeros((32, 64), BF16)
    zero256 = jnp.zeros((32, 256), BF16)
    for k in range(3):
        head, tail = parts[k][:, :256], parts[k][:, 256:]
        heads = [head if j <= 2 - k else zero256 for j in range(3)]
        tails = [tail if j <= 2 - k else zero64 for j in range(3)]
        c3[32 * k:32 * k + 32, :] = jnp.concatenate(heads + tails + [zero64], axis=1)
    own = jnp.transpose(c_ref[pl.ds(pl.multiple_of(o * 80, 8), 80), :])
    for m in range(80):
        cb[m] = jnp.broadcast_to(own[:, m:m + 1], (32, 128))
    stage[1] = jnp.zeros((512, 128), F32)
    gam[...] = jnp.zeros((32, 256), F32)

    m_copy.wait()
    m0, m1, m2 = split3(mown[...])
    pad = jnp.zeros((32, 896), BF16)
    mall[pl.ds(a, 1), 0:224, :] = m0[None]
    mall[pl.ds(a, 1), 224:256, :] = pad[None]
    mall[4, 0:224, :] = m1
    mall[4, 224:256, :] = pad
    mall[5, 0:224, :] = m2
    mall[5, 224:256, :] = pad

    pl.semaphore_wait(barrier, 15)

    quarter = pl.ds(pl.multiple_of(o * 64, 64), 64)

    def mz_copy(j):
        return remote(mall.at[a, quarter, :], mall.at[a, quarter, :], mz_send.at[j], mz_recv.at[a], (planes[j], o))

    for j in range(3):
        mz_copy(j).start()

    def mf_copy(j, k):
        part = mall.at[planes[j], quarter, :]
        return remote(part, part, mf_send.at[j, k], mf_recv.at[planes[j], o], (a, (o + k + 1) % 4))

    def half_copy(ii, dest, rows):
        d = dest[0] * 4 + dest[1]
        return remote(sbuf.at[2 * d + ii, rows, :], rbuf.at[ii, me, rows, :], s_send.at[ii, d], s_recv.at[ii, me], dest)

    def group(g, carry):
        for cp in b_copies(g):
            cp.wait()

        @pl.when(g + AHEAD < 10)
        def _():
            for cp in b_copies(g + AHEAD):
                cp.start()

        slot = lax.rem(g, SLOTS)
        b_tail = bb.at[2, g].reshape(1792, 128)
        b_tail[:, 0:64] = b3.at[slot].reshape(1792, 64)[...]
        views = [bb.at[t, g].reshape(1792, 128) for t in range(3)]
        base = lax.rem(g, 2) * 8

        def row(m, carry):
            x0, x1, x2 = [split3(v[pl.ds(m, 224, stride=8), :]) for v in views]
            z = jnp.zeros((224, 64), BF16)
            w = jnp.concatenate([x0[0], x1[0], x0[1], x1[1], x0[2], x1[2],
                                 x2[0][:, :64], x2[1][:, :64], x2[2][:, :64], z], axis=1)
            r = dot_nt(c3[...], w)
            h = r[0:32] + r[32:64] + r[64:96]
            stage[0, pl.ds(base + m, 32, stride=16), :] = h[:, :128]
            stage[1, pl.ds(base + m, 32, stride=16), 0:96] = h[:, 128:]
            coef = cb[g * 8 + m]
            gam[:, 0:128] += h[:, :128] * coef
            gam[:, 128:224] += h[:, 128:] * coef[:, :96]
            return carry

        lax.fori_loop(0, 8, row, 0)

        @pl.when(lax.rem(g, 2) == 1)
        def _():
            rows = pl.ds(pl.multiple_of((g // 2) * 16, 16), 16)
            for t in range(2):
                sbuf[:, rows, 128 * t:128 * t + 128] = stage[t].reshape(32, 16, 128).astype(BF16)
            for dest in peers:
                half_copy(0, dest, rows).start()

        @pl.when(g == 3)
        def _():
            for j in range(3):
                remote(mall.at[planes[j], quarter, :], mall.at[planes[j], quarter, :], mz_send.at[j],
                       mz_recv.at[planes[j]], (planes[j], o)).wait_recv()
                for k in range(3):
                    mf_copy(j, k).start()

        return carry

    lax.fori_loop(0, 10, group, 0)

    full = pl.ds(0, 80)
    for dest in peers:
        half_copy(1, dest, full).start()
    rbuf[:, pl.ds(me, 1)] = sbuf[pl.ds(2 * me, 2)][:, None]

    def g_copy(dest):
        return remote(gsend, grecv.at[me], g_send.at[dest[0] * 4 + dest[1]], g_recv.at[me], dest)

    g_row = jnp.sum(gam[...], axis=0, keepdims=True)
    gsend[...] = g_row
    grecv[pl.ds(me, 1)] = g_row[None]
    for dest in peers:
        g_copy(dest).start()

    def lanes_of(rows):
        return jnp.concatenate([r[:, :224] for r in rows], axis=1)

    def times_metric(row):
        return jnp.sum(mown[...] * row, axis=1, keepdims=True)

    for s in peers:
        remote(gsend, grecv.at[s[0] * 4 + s[1]], g_send.at[0], g_recv.at[s[0] * 4 + s[1]], s).wait_recv()
    gamma = lanes_of([grecv[4 * b] + grecv[4 * b + 1] + grecv[4 * b + 2] + grecv[4 * b + 3] for b in range(4)])
    fit = jnp.broadcast_to(times_metric(gamma), (224, 128))
    fit_row = jnp.concatenate([jnp.transpose(fit[:128])[0:1], jnp.transpose(fit[96:])[0:1, 32:], jnp.zeros((1, 32), F32)],
                              axis=1)
    fsend[...] = fit_row
    frecv[pl.ds(a, 1)] = fit_row[None]

    def f_copy(j):
        return remote(fsend, frecv.at[a], f_send.at[j], f_recv.at[a], (planes[j], o))

    for j in range(3):
        f_copy(j).start()
    for j in range(3):
        remote(fsend, frecv.at[planes[j]], f_send.at[j], f_recv.at[planes[j]], (planes[j], o)).wait_recv()
    weights = times_metric(lanes_of([frecv[b] for b in range(4)]))
    wb[...] = jnp.broadcast_to(2.0 * weights, (224, 128))

    def coul(q, acc):
        w = jnp.broadcast_to(wb[pl.ds(q, 1), :], (8, 128))
        return tuple(acc[t * 10 + g] + w * bb[t, g, q] for t in range(3) for g in range(10))

    acc = lax.fori_loop(0, 224, coul, tuple(jnp.zeros((8, 128), F32) for _ in range(30)))
    for g in range(10):
        jacc[8 * g:8 * g + 8, :] = jnp.concatenate([acc[g], acc[10 + g], acc[20 + g][:, :64]], axis=1)

    for j in range(3):
        for k in range(3):
            po = (o + k + 1) % 4
            part = mall.at[planes[j], pl.ds(pl.multiple_of(po * 64, 64), 64), :]
            remote(part, part, mf_send.at[j, k], mf_recv.at[planes[j], po], (a, po)).wait_recv()

    for ii in range(2):
        for s in peers:
            n = s[0] * 4 + s[1]
            remote(sbuf.at[ii], rbuf.at[ii, n], s_send.at[ii, n], s_recv.at[ii, n], s).wait_recv()
        for n0, n1 in ((0, 256), (256, 512), (512, 768), (768, 896)):
            t = dot(rbuf[ii, 0:4].reshape(320, 256), mall[0, :, n0:n1])
            for b in range(1, 4):
                t += dot(rbuf[ii, 4 * b:4 * b + 4].reshape(320, 256), mall[b, :, n0:n1])
            mine = rbuf[ii, pl.ds(a * 4, 4)].reshape(320, 256)
            t += dot(mine, mall[4, :, n0:n1]) + dot(mine, mall[5, :, n0:n1])
            for k, h in enumerate(split3(t)):
                tt[k, :, n0:n1] = h
        t0, t1, t2 = tt[0], tt[1], tt[2]
        k = dot_nt(t0, t0) + dot_nt(t1, t1) + dot_nt(t0, t1) + dot_nt(t0, t2) + dot_nt(t1, t0) + dot_nt(t2, t0)
        if ii == 0:
            ks[...] = k
        else:
            ks[...] += k

    for c in range(4):
        gs[:, c] = -ks[:, 80 * c:80 * c + 80].reshape(4, 80, 80)
        gs[pl.ds(o, 1), c] += jacc[:, 80 * c:80 * c + 80][None]

    def r_copy(dest):
        return remote(gs.at[dest[1], dest[0]], gr.at[me], r_send.at[dest[0] * 4 + dest[1]], r_recv.at[me], dest)

    for dest in peers:
        r_copy(dest).start()
    total = gs[o, a]
    for s in peers:
        n = s[0] * 4 + s[1]
        remote(gs.at[s[1], s[0]], gr.at[n], r_send.at[n], r_recv.at[n], s).wait_recv()
        total = total + gr[n]
    out_ref[0] = total

    for dest in peers:
        half_copy(0, dest, full).wait_send()
        half_copy(1, dest, full).wait_send()
        g_copy(dest).wait_send()
        r_copy(dest).wait_send()
    for j in range(3):
        mz_copy(j).wait_send()
        f_copy(j).wait_send()
        for k in range(3):
            mf_copy(j, k).wait_send()


def solution(mesh):
    def local_fock(ints_blk, metric_blk, orbitals):
        dma = pltpu.SemaphoreType.DMA
        return pl.pallas_call(
            kernel,
            name='fock',
            out_shape=jax.ShapeDtypeStruct((1, 80, 80), F32),
            in_specs=[pl.BlockSpec(memory_space=pl.ANY), pl.BlockSpec(memory_space=pl.ANY),
                      pl.BlockSpec(memory_space=pltpu.VMEM)],
            out_specs=pl.BlockSpec(memory_space=pltpu.VMEM),
            scratch_shapes=[
                pltpu.VMEM((3, 10, 224, 8, 128), F32),
                pltpu.VMEM((SLOTS, 224, 8, 64), F32),
                pltpu.VMEM((2, 512, 128), F32),
                pltpu.VMEM((32, 80, 256), BF16),
                pltpu.VMEM((2, 16, 80, 256), BF16),
                pltpu.VMEM((6, 256, 896), BF16),
                pltpu.VMEM((224, 896), F32),
                pltpu.VMEM((80, 32, 128), F32),
                pltpu.VMEM((96, 1024), BF16),
                pltpu.VMEM((3, 320, 896), BF16),
                pltpu.VMEM((320, 320), F32),
                pltpu.VMEM((80, 320), F32),
                pltpu.VMEM((32, 256), F32),
                pltpu.VMEM((1, 256), F32),
                pltpu.VMEM((16, 1, 256), F32),
                pltpu.VMEM((1, 256), F32),
                pltpu.VMEM((4, 1, 256), F32),
                pltpu.VMEM((224, 128), F32),
                pltpu.VMEM((4, 4, 80, 80), F32),
                pltpu.VMEM((16, 80, 80), F32),
                dma((3, SLOTS)), dma(()),
                dma((2, 16)), dma((2, 16)),
                dma((3,)), dma((4,)),
                dma((3, 3)), dma((4, 4)),
                dma((16,)), dma((16,)),
                dma((3,)), dma((4,)),
                dma((16,)), dma((16,)),
            ],
            compiler_params=pltpu.CompilerParams(collective_id=0, has_side_effects=True, vmem_limit_bytes=67043328),
        )(ints_blk, metric_blk, orbitals[0])

    return jax.shard_map(local_fock, mesh=mesh, in_specs=(P(('sys', 'aux'), 'orb', None), P(('sys', 'aux'), None), P('sys', None, None)), out_specs=P('sys', 'orb', 'aux'), check_vma=False)
```

```python
import functools

import jax
import jax.numpy as jnp
from jax import lax
from jax.experimental import pallas as pl
from jax.experimental.pallas import tpu as pltpu
from jax.sharding import PartitionSpec as P

F32, BF16 = jnp.float32, jnp.bfloat16
MESH = pl.DeviceIdType.MESH
NT = (((1,), (1,)), ((), ()))
AHEAD = 4


def split3(x):
    h0 = x.astype(BF16)
    r1 = x - h0.astype(F32)
    h1 = r1.astype(BF16)
    r2 = r1 - h1.astype(F32)
    return h0, h1, r2.astype(BF16)


def dot(a, b):
    return jnp.dot(a, b, preferred_element_type=F32)


def dot_nt(a, b):
    return lax.dot_general(a, b, NT, preferred_element_type=F32)


def kernel(b_hbm, m_hbm, c_ref, out_ref, bb, stage, sbuf, rbuf, mall, mown, cb, c3, tt, ks, jacc, gam, gsend, grecv,
           fsend, frecv, gs, gr, b_sem, m_sem, s_send, s_recv, mz_send, mz_recv, mf_send, mf_recv, g_send, g_recv,
           f_send, f_recv, r_send, r_recv):
    a, o = lax.axis_index('aux'), lax.axis_index('orb')
    me = a * 4 + o
    planes = [(a + 2) % 4, 3 - a, a + 1 - 2 * (a % 2), a]
    peers = [(planes[k // 4], (o + k % 4) % 4) for k in range(16) if k != 12]

    def remote(src, dst, send, recv, dest):
        return pltpu.make_async_remote_copy(src_ref=src, dst_ref=dst, send_sem=send, recv_sem=recv,
                                            device_id={'aux': dest[0], 'orb': dest[1]}, device_id_type=MESH)

    def b_copy(g):
        rows = pl.ds(g * 4, 4)
        return pltpu.make_async_copy(b_hbm.at[rows], bb.at[rows], b_sem.at[g])

    for g in range(AHEAD):
        b_copy(g).start()
    m_copy = pltpu.make_async_copy(m_hbm, mown, m_sem)
    m_copy.start()

    barrier = pltpu.get_barrier_semaphore()
    for dest in peers:
        pl.semaphore_signal(barrier, inc=1, device_id={'aux': dest[0], 'orb': dest[1]}, device_id_type=MESH)

    parts = split3(c_ref[...])
    zero = jnp.zeros((32, 320), BF16)
    for k in range(3):
        rows = [parts[k] if j <= 2 - k else zero for j in range(3)]
        c3[32 * k:32 * k + 32, :] = jnp.concatenate(rows + [zero[:, :64]], axis=1)
    own = jnp.zeros((32, 80), F32)
    for k in range(4):
        own = jnp.where(o == k, c_ref[:, 80 * k:80 * k + 80], own)
    for m in range(80):
        cb[m] = jnp.broadcast_to(own[:, m:m + 1], (32, 128))
    stage[1] = jnp.zeros((512, 128), F32)
    gam[...] = jnp.zeros((32, 256), F32)

    m_copy.wait()
    m0, m1, m2 = split3(mown[...])
    pad = jnp.zeros((32, 896), BF16)
    mall[pl.ds(a, 1), 0:224, :] = m0[None]
    mall[pl.ds(a, 1), 224:256, :] = pad[None]
    mall[4, 0:224, :] = m1
    mall[4, 224:256, :] = pad
    mall[5, 0:224, :] = m2
    mall[5, 224:256, :] = pad

    pl.semaphore_wait(barrier, 15)

    quarter = pl.ds(pl.multiple_of(o * 64, 64), 64)

    def mz_copy(plane, step):
        part = mall.at[plane, quarter, :]
        return remote(part, part, mz_send.at[plane, (step + 1) // 2], mz_recv.at[plane], (a + step, o))

    def relay(r, action):
        for step in (1, -1):
            plane = a - step * r

            @pl.when((plane >= 0) & (plane <= 3))
            def _():
                if action == 'send' and r > 0:
                    mz_copy(plane, step).wait_recv()

                @pl.when((a + step >= 0) & (a + step <= 3))
                def _():
                    if r < 3:
                        cp = mz_copy(plane, step)
                        cp.start() if action == 'send' else cp.wait_send()

    relay(0, 'send')

    def mf_copy(j, k):
        part = mall.at[planes[j], quarter, :]
        return remote(part, part, mf_send.at[j, k], mf_recv.at[planes[j], o], (a, (o + k + 1) % 4))

    def half_copy(ii, dest, rows):
        d = dest[0] * 4 + dest[1]
        return remote(sbuf.at[2 * d + ii, rows, :], rbuf.at[ii, me, rows, :], s_send.at[ii, d], s_recv.at[ii, me], dest)

    def group(g, carry):
        for k in range(2):
            b_copy(2 * g + k).wait()

        @pl.when(2 * g + AHEAD < 20)
        def _():
            for k in range(2):
                b_copy(2 * g + k + AHEAD).start()

        base = lax.rem(g, 2) * 8

        def row(m, carry):
            w = jnp.concatenate(list(split3(bb[g * 8 + m])) + [jnp.zeros((64, 224), BF16)], axis=0)
            r = dot(c3[...], w)
            h = r[0:32] + r[32:64] + r[64:96]
            stage[0, pl.ds(base + m, 32, stride=16), :] = h[:, :128]
            stage[1, pl.ds(base + m, 32, stride=16), 0:96] = h[:, 128:]
            coef = cb[g * 8 + m]
            gam[:, 0:128] += h[:, :128] * coef
            gam[:, 128:224] += h[:, 128:] * coef[:, :96]
            return carry

        lax.fori_loop(0, 8, row, 0)

        @pl.when(lax.rem(g, 2) == 1)
        def _():
            rows = pl.ds(pl.multiple_of((g // 2) * 16, 16), 16)
            for t in range(2):
                sbuf[:, rows, 128 * t:128 * t + 128] = stage[t].reshape(32, 16, 128).astype(BF16)
            for dest in peers:
                half_copy(0, dest, rows).start()

        for r in (1, 2):
            @pl.when(g == 4 * r)
            def _():
                relay(r, 'send')

        return carry

    lax.fori_loop(0, 10, group, 0)

    def g_copy(dest):
        return remote(gsend, grecv.at[me], g_send.at[dest[0] * 4 + dest[1]], g_recv.at[me], dest)

    g_row = jnp.sum(gam[...], axis=0, keepdims=True)
    gsend[...] = g_row
    grecv[pl.ds(me, 1)] = g_row[None]
    for dest in peers:
        g_copy(dest).start()

    full = pl.ds(0, 80)
    for dest in peers:
        half_copy(1, dest, full).start()
    rbuf[:, pl.ds(me, 1)] = sbuf[pl.ds(2 * me, 2)][:, None]

    relay(3, 'send')
    for j in range(3):
        for k in range(3):
            mf_copy(j, k).start()

    def lanes_of(rows):
        return jnp.concatenate([r[:, :224] for r in rows], axis=1)

    def as_row(col):
        x = jnp.broadcast_to(col, (224, 128))
        return jnp.concatenate([jnp.transpose(x[:128])[0:1], jnp.transpose(x[96:])[0:1, 32:], jnp.zeros((1, 32), F32)],
                               axis=1)

    def times_metric(row):
        return jnp.sum(mown[...] * row, axis=1, keepdims=True)

    for s in peers:
        remote(gsend, grecv.at[s[0] * 4 + s[1]], g_send.at[0], g_recv.at[s[0] * 4 + s[1]], s).wait_recv()
    gamma = lanes_of([grecv[4 * b] + grecv[4 * b + 1] + grecv[4 * b + 2] + grecv[4 * b + 3] for b in range(4)])
    fit_row = as_row(times_metric(gamma))
    fsend[...] = fit_row
    frecv[pl.ds(a, 1)] = fit_row[None]

    def f_copy(j):
        return remote(fsend, frecv.at[a], f_send.at[j], f_recv.at[a], (planes[j], o))

    for j in range(3):
        f_copy(j).start()
    for j in range(3):
        remote(fsend, frecv.at[planes[j]], f_send.at[j], f_recv.at[planes[j]], (planes[j], o)).wait_recv()
    weights = times_metric(lanes_of([frecv[b] for b in range(4)]))
    w_row = as_row(2.0 * weights)

    lane = lax.broadcasted_iota(jnp.int32, (320, 80), 1)

    def coul(m, acc):
        x = bb[m]
        col = jnp.sum(x[:, :128] * w_row[:, :128], axis=1, keepdims=True) + jnp.sum(
            x[:, 128:] * w_row[:, 128:224], axis=1, keepdims=True)
        return jnp.where(lane == m, col, acc)

    jacc[...] = lax.fori_loop(0, 80, coul, jnp.zeros((320, 80), F32))
    jt = jnp.transpose(jacc[...])

    for j in range(3):
        for k in range(3):
            po = (o + k + 1) % 4
            part = mall.at[planes[j], pl.ds(pl.multiple_of(po * 64, 64), 64), :]
            remote(part, part, mf_send.at[j, k], mf_recv.at[planes[j], po], (a, po)).wait_recv()

    for ii in range(2):
        for s in peers:
            n = s[0] * 4 + s[1]
            remote(sbuf.at[ii], rbuf.at[ii, n], s_send.at[ii, n], s_recv.at[ii, n], s).wait_recv()
        for n0, n1 in ((0, 256), (256, 512), (512, 768), (768, 896)):
            t = dot(rbuf[ii, 0:4].reshape(320, 256), mall[0, :, n0:n1])
            for b in range(1, 4):
                t += dot(rbuf[ii, 4 * b:4 * b + 4].reshape(320, 256), mall[b, :, n0:n1])
            mine = rbuf[ii, pl.ds(a * 4, 4)].reshape(320, 256)
            t += dot(mine, mall[4, :, n0:n1]) + dot(mine, mall[5, :, n0:n1])
            for k, h in enumerate(split3(t)):
                tt[k, :, n0:n1] = h
        t0, t1, t2 = tt[0], tt[1], tt[2]
        k = dot_nt(t0, t0) + dot_nt(t1, t1) + dot_nt(t0, t1) + dot_nt(t0, t2) + dot_nt(t1, t0) + dot_nt(t2, t0)
        if ii == 0:
            ks[...] = k
        else:
            ks[...] += k

    for c in range(4):
        gs[:, c] = -ks[:, 80 * c:80 * c + 80].reshape(4, 80, 80)
        gs[pl.ds(o, 1), c] += jt[:, 80 * c:80 * c + 80][None]

    def r_copy(dest):
        return remote(gs.at[dest[1], dest[0]], gr.at[me], r_send.at[dest[0] * 4 + dest[1]], r_recv.at[me], dest)

    for dest in peers:
        r_copy(dest).start()
    total = gs[o, a]
    for s in peers:
        n = s[0] * 4 + s[1]
        remote(gs.at[s[1], s[0]], gr.at[n], r_send.at[n], r_recv.at[n], s).wait_recv()
        total = total + gr[n]
    out_ref[0] = total

    for dest in peers:
        half_copy(0, dest, full).wait_send()
        half_copy(1, dest, full).wait_send()
        g_copy(dest).wait_send()
        r_copy(dest).wait_send()
    for r in range(3):
        relay(r, 'drain')
    for j in range(3):
        f_copy(j).wait_send()
        for k in range(3):
            mf_copy(j, k).wait_send()


def solution(mesh):
    def local_fock(ints_blk, metric_blk, orbitals):
        dma = pltpu.SemaphoreType.DMA
        return pl.pallas_call(
            kernel,
            name='fock',
            out_shape=jax.ShapeDtypeStruct((1, 80, 80), F32),
            in_specs=[pl.BlockSpec(memory_space=pl.ANY), pl.BlockSpec(memory_space=pl.ANY),
                      pl.BlockSpec(memory_space=pltpu.VMEM)],
            out_specs=pl.BlockSpec(memory_space=pltpu.VMEM),
            scratch_shapes=[
                pltpu.VMEM((80, 320, 224), F32),
                pltpu.VMEM((2, 512, 128), F32),
                pltpu.VMEM((32, 80, 256), BF16),
                pltpu.VMEM((2, 16, 80, 256), BF16),
                pltpu.VMEM((6, 256, 896), BF16),
                pltpu.VMEM((224, 896), F32),
                pltpu.VMEM((80, 32, 128), F32),
                pltpu.VMEM((96, 1024), BF16),
                pltpu.VMEM((3, 320, 896), BF16),
                pltpu.VMEM((320, 320), F32),
                pltpu.VMEM((320, 80), F32),
                pltpu.VMEM((32, 256), F32),
                pltpu.VMEM((1, 256), F32),
                pltpu.VMEM((16, 1, 256), F32),
                pltpu.VMEM((1, 256), F32),
                pltpu.VMEM((4, 1, 256), F32),
                pltpu.VMEM((4, 4, 80, 80), F32),
                pltpu.VMEM((16, 80, 80), F32),
                dma((20,)), dma(()),
                dma((2, 16)), dma((2, 16)),
                dma((4, 2)), dma((4,)),
                dma((3, 3)), dma((4, 4)),
                dma((16,)), dma((16,)),
                dma((3,)), dma((4,)),
                dma((16,)), dma((16,)),
            ],
            compiler_params=pltpu.CompilerParams(collective_id=0, has_side_effects=True, vmem_limit_bytes=67043328),
        )(jnp.transpose(ints_blk, (1, 2, 0)), metric_blk, jnp.transpose(orbitals[0]))

    return jax.shard_map(local_fock, mesh=mesh, in_specs=(P(('sys', 'aux'), 'orb', None), P(('sys', 'aux'), None), P('sys', None, None)), out_specs=P('sys', 'orb', 'aux'), check_vma=False)
```

```python
import functools

import jax
import jax.numpy as jnp
from jax import lax
from jax.experimental import pallas as pl
from jax.experimental.pallas import tpu as pltpu
from jax.sharding import PartitionSpec as P

F32, BF16 = jnp.float32, jnp.bfloat16
MESH = pl.DeviceIdType.MESH
NT = (((1,), (1,)), ((), ()))
AHEAD = 4


def split3(x):
    h0 = x.astype(BF16)
    r1 = x - h0.astype(F32)
    h1 = r1.astype(BF16)
    r2 = r1 - h1.astype(F32)
    return h0, h1, r2.astype(BF16)


def dot(a, b):
    return jnp.dot(a, b, preferred_element_type=F32)


def dot_nt(a, b):
    return lax.dot_general(a, b, NT, preferred_element_type=F32)


def kernel(b_hbm, m_hbm, c_ref, out_ref, bb, stage, sbuf, rbuf, mall, mown, cb, c3, tt, ks, jacc, gam, gsend, grecv,
           fsend, frecv, gs, gp, gf, gr, b_sem, m_sem, s_send, s_recv, mz_send, mz_recv, mf_send, mf_recv, g_send, g_recv,
           f_send, f_recv, p_sems, r_send, r_recv):
    a, o = lax.axis_index('aux'), lax.axis_index('orb')
    me = a * 4 + o
    core, row_y = o % 2, o // 2
    core_mate, y_mate = o + 1 - 2 * core, (o + 2) % 4
    planes = [(a + 2) % 4, 3 - a, a + 1 - 2 * (a % 2), a]
    peers = [(planes[k // 4], (o + k % 4) % 4) for k in range(16) if k != 12]

    def remote(src, dst, send, recv, dest):
        return pltpu.make_async_remote_copy(src_ref=src, dst_ref=dst, send_sem=send, recv_sem=recv,
                                            device_id={'aux': dest[0], 'orb': dest[1]}, device_id_type=MESH)

    def b_copy(g):
        rows = pl.ds(g * 4, 4)
        return pltpu.make_async_copy(b_hbm.at[rows], bb.at[rows], b_sem.at[g])

    m_copy = pltpu.make_async_copy(m_hbm, mown, m_sem)
    m_copy.start()
    for g in range(AHEAD):
        b_copy(g).start()

    barrier = pltpu.get_barrier_semaphore()
    for dest in peers:
        pl.semaphore_signal(barrier, inc=1, device_id={'aux': dest[0], 'orb': dest[1]}, device_id_type=MESH)

    m_copy.wait()
    m0, m1, m2 = split3(mown[...])
    pad = jnp.zeros((32, 896), BF16)
    mall[pl.ds(a, 1), 0:224, :] = m0[None]
    mall[pl.ds(a, 1), 224:256, :] = pad[None]
    mall[4, 0:224, :] = m1
    mall[4, 224:256, :] = pad
    mall[5, 0:224, :] = m2
    mall[5, 224:256, :] = pad

    pl.semaphore_wait(barrier, 15)

    quarter = pl.ds(pl.multiple_of(o * 64, 64), 64)

    def mz_copy(plane, step):
        part = mall.at[plane, quarter, :]
        return remote(part, part, mz_send.at[plane, (step + 1) // 2], mz_recv.at[plane], (a + step, o))

    def mf_copy(plane, part_of, dest, k):
        part = mall.at[plane, pl.ds(pl.multiple_of(part_of * 64, 64), 64), :]
        return remote(part, part, mf_send.at[plane, k], mf_recv.at[plane, part_of], (a, dest))

    def relay(r, action):
        for step in (1, -1):
            plane = a - step * r

            @pl.when((plane >= 0) & (plane <= 3))
            def _():
                if action == 'send' and r > 0:
                    mz_copy(plane, step).wait_recv()
                if r < 3:
                    @pl.when((a + step >= 0) & (a + step <= 3))
                    def _():
                        cp = mz_copy(plane, step)
                        cp.start() if action == 'send' else cp.wait_send()
                if action == 'send' and r > 0:
                    mf_copy(plane, o, core_mate, 0).start()
                    mf_copy(plane, o, y_mate, 1).start()

    def pass_on(r):
        for step in (1, -1):
            plane = a - step * r

            @pl.when((plane >= 0) & (plane <= 3))
            def _():
                mf_copy(plane, y_mate, y_mate, 2).wait_recv()
                mf_copy(plane, y_mate, core_mate, 2).start()

    relay(0, 'send')

    def half_copy(ii, dest, rows):
        d = dest[0] * 4 + dest[1]
        return remote(sbuf.at[2 * d + ii, rows, :], rbuf.at[ii, me, rows, :], s_send.at[ii, d], s_recv.at[ii, me], dest)

    parts = split3(c_ref[...])
    zero = jnp.zeros((32, 320), BF16)
    for k in range(3):
        rows = [parts[k] if j <= 2 - k else zero for j in range(3)]
        c3[32 * k:32 * k + 32, :] = jnp.concatenate(rows + [zero[:, :64]], axis=1)
    own = jnp.zeros((32, 80), F32)
    for k in range(4):
        own = jnp.where(o == k, c_ref[:, 80 * k:80 * k + 80], own)
    for m in range(80):
        cb[m] = jnp.broadcast_to(own[:, m:m + 1], (32, 128))
    stage[1] = jnp.zeros((512, 128), F32)
    gam[...] = jnp.zeros((32, 256), F32)

    def group(g, carry):
        for k in range(2):
            b_copy(2 * g + k).wait()

        @pl.when(2 * g + AHEAD < 20)
        def _():
            for k in range(2):
                b_copy(2 * g + k + AHEAD).start()

        base = lax.rem(g, 2) * 8

        def rows4(k, carry):
            part0 = part1 = None
            for j in range(4):
                m = 4 * k + j
                w = jnp.concatenate(list(split3(bb[g * 8 + m])) + [jnp.zeros((64, 224), BF16)], axis=0)
                r = dot(c3[...], w)
                h = r[0:32] + r[32:64] + r[64:96]
                stage[0, pl.ds(base + m, 32, stride=16), :] = h[:, :128]
                stage[1, pl.ds(base + m, 32, stride=16), 0:96] = h[:, 128:]
                coef = cb[g * 8 + m]
                add0, add1 = h[:, :128] * coef, h[:, 128:] * coef[:, :96]
                part0 = add0 if part0 is None else part0 + add0
                part1 = add1 if part1 is None else part1 + add1
            gam[:, 0:128] += part0
            gam[:, 128:224] += part1
            return carry

        lax.fori_loop(0, 2, rows4, 0)

        @pl.when(lax.rem(g, 2) == 1)
        def _():
            rows = pl.ds(pl.multiple_of((g // 2) * 16, 16), 16)
            for t in range(2):
                sbuf[:, rows, 128 * t:128 * t + 128] = stage[t].reshape(32, 16, 128).astype(BF16)
            for dest in peers:
                half_copy(0, dest, rows).start()

        @pl.when(g == 3)
        def _():
            relay(1, 'send')

        @pl.when(g == 6)
        def _():
            relay(2, 'send')
            pass_on(1)

        return carry

    lax.fori_loop(0, 10, group, 0)

    def g_copy(dest):
        return remote(gsend, grecv.at[me], g_send.at[dest[0] * 4 + dest[1]], g_recv.at[me], dest)

    g_row = jnp.sum(gam[...], axis=0, keepdims=True)
    gsend[...] = g_row
    grecv[pl.ds(me, 1)] = g_row[None]
    for dest in peers:
        g_copy(dest).start()

    full = pl.ds(0, 80)
    for dest in peers:
        half_copy(1, dest, pl.ds(0, 48)).start()
    rbuf[:, pl.ds(me, 1)] = sbuf[pl.ds(2 * me, 2)][:, None]
    relay(3, 'send')
    pass_on(2)

    def lanes_of(rows):
        return jnp.concatenate([r[:, :224] for r in rows], axis=1)

    def as_row(col):
        x = jnp.broadcast_to(col, (224, 128))
        return jnp.concatenate([jnp.transpose(x[:128])[0:1], jnp.transpose(x[96:])[0:1, 32:], jnp.zeros((1, 32), F32)],
                               axis=1)

    def times_metric(row):
        return jnp.sum(mown[...] * row, axis=1, keepdims=True)

    for s in peers:
        remote(gsend, grecv.at[s[0] * 4 + s[1]], g_send.at[0], g_recv.at[s[0] * 4 + s[1]], s).wait_recv()
    gamma = lanes_of([grecv[4 * b] + grecv[4 * b + 1] + grecv[4 * b + 2] + grecv[4 * b + 3] for b in range(4)])
    fit_row = as_row(times_metric(gamma))
    fsend[...] = fit_row
    frecv[pl.ds(a, 1)] = fit_row[None]

    def f_copy(j):
        return remote(fsend, frecv.at[a], f_send.at[j], f_recv.at[a], (planes[j], o))

    for j in range(3):
        f_copy(j).start()
    for dest in peers:
        half_copy(1, dest, pl.ds(48, 32)).start()
    pass_on(3)

    for r in range(1, 4):
        for step in (1, -1):
            plane = a - step * r

            @pl.when((plane >= 0) & (plane <= 3))
            def _():
                for part_of in (core_mate, 3 - o):
                    mf_copy(plane, part_of, part_of, 0).wait_recv()

    def t_and_k(ii):
        for s in peers:
            n = s[0] * 4 + s[1]
            remote(sbuf.at[ii], rbuf.at[ii, n], s_send.at[ii, n], s_recv.at[ii, n], s).wait_recv()
        for n0, n1 in ((0, 256), (256, 512), (512, 768), (768, 896)):
            t = dot(rbuf[ii, 0:4].reshape(320, 256), mall[0, :, n0:n1])
            for b in range(1, 4):
                t += dot(rbuf[ii, 4 * b:4 * b + 4].reshape(320, 256), mall[b, :, n0:n1])
            mine = rbuf[ii, pl.ds(a * 4, 4)].reshape(320, 256)
            t += dot(mine, mall[4, :, n0:n1]) + dot(mine, mall[5, :, n0:n1])
            for k, h in enumerate(split3(t)):
                tt[k, :, n0:n1] = h
        t0, t1, t2 = tt[0], tt[1], tt[2]
        k = dot_nt(t0, t0) + dot_nt(t1, t1) + dot_nt(t0, t1) + dot_nt(t0, t2) + dot_nt(t1, t0) + dot_nt(t2, t0)
        if ii == 0:
            ks[...] = k
        else:
            ks[...] += k

    t_and_k(0)
    for j in range(3):
        remote(fsend, frecv.at[planes[j]], f_send.at[j], f_recv.at[planes[j]], (planes[j], o)).wait_recv()
    weights = times_metric(lanes_of([frecv[b] for b in range(4)]))
    w_row = as_row(2.0 * weights)

    lane = lax.broadcasted_iota(jnp.int32, (8, 128), 1)
    w0, w1 = jnp.broadcast_to(w_row[:, :128], (8, 128)), jnp.broadcast_to(w_row[:, 128:224], (8, 96))

    def coul(k, carry):
        rows = pl.ds(pl.multiple_of(k * 8, 8), 8)
        acc = jnp.zeros((8, 128), F32)
        for m in range(80):
            y = bb[m, rows, 0:128] * w0
            z = bb[m, rows, 128:224] * w1
            col = jnp.sum(y, axis=1, keepdims=True) + jnp.sum(z, axis=1, keepdims=True)
            acc = jnp.where(lane == m, col, acc)
        jacc[rows, :] = acc[:, :80]
        return carry

    lax.fori_loop(0, 40, coul, 0)
    jt = jnp.transpose(jacc[...])

    t_and_k(1)

    def packed(x):
        tail = jnp.concatenate([x[56:, :48], jnp.concatenate([x[56:, 48:], jnp.zeros((24, 16), F32)], axis=1),
                                jnp.zeros((8, 48), F32)], axis=0)
        return jnp.concatenate([x[:56], tail], axis=1)

    for c in range(4):
        for k in range(4):
            gs[k % 2, k // 2, c] = packed(jnp.where(o == k, jt[:, 80 * c:80 * c + 80], 0.0)
                                          - ks[80 * k:80 * k + 80, 80 * c:80 * c + 80])
    pair = remote(gs.at[1 - core], gp, p_sems.at[0], p_sems.at[1], (a, core_mate))
    pair.start()
    pair.wait()
    gf[...] = gs[core] + gp[...]

    def r_copy(k):
        plane, y = planes[k // 2], (row_y + k % 2) % 2
        return remote(gf.at[y, plane], gr.at[a, row_y], r_send.at[k], r_recv.at[a, row_y], (plane, 2 * y + core))

    r_order = (0, 1, 2, 3, 4, 5, 7)
    for k in r_order:
        r_copy(k).start()
    total = gf[row_y, a]
    for k in r_order:
        plane, y = planes[k // 2], (row_y + k % 2) % 2
        remote(gf.at[y, plane], gr.at[plane, y], r_send.at[k], r_recv.at[plane, y], (plane, 2 * y + core)).wait_recv()
        total = total + gr[plane, y]
    out_ref[0] = jnp.concatenate([total[:, :80], jnp.concatenate([total[0:24, 80:128], total[24:48, 80:112]], axis=1)], axis=0)


    for dest in peers:
        half_copy(0, dest, full).wait_send()
        half_copy(1, dest, full).wait_send()
        g_copy(dest).wait_send()
    for k in r_order:
        r_copy(k).wait_send()
    for r in range(3):
        relay(r, 'drain')
    for j in range(3):
        f_copy(j).wait_send()
        for k in range(3):
            mf_copy(planes[j], o, o, k).wait_send()


def solution(mesh):
    def local_fock(ints_blk, metric_blk, orbitals):
        dma = pltpu.SemaphoreType.DMA
        return pl.pallas_call(
            kernel,
            name='fock',
            out_shape=jax.ShapeDtypeStruct((1, 80, 80), F32),
            in_specs=[pl.BlockSpec(memory_space=pl.ANY), pl.BlockSpec(memory_space=pl.ANY),
                      pl.BlockSpec(memory_space=pltpu.VMEM)],
            out_specs=pl.BlockSpec(memory_space=pltpu.VMEM),
            scratch_shapes=[
                pltpu.VMEM((80, 320, 224), F32),
                pltpu.VMEM((2, 512, 128), F32),
                pltpu.VMEM((32, 80, 256), BF16),
                pltpu.VMEM((2, 16, 80, 256), BF16),
                pltpu.VMEM((6, 256, 896), BF16),
                pltpu.VMEM((224, 896), F32),
                pltpu.VMEM((80, 32, 128), F32),
                pltpu.VMEM((96, 1024), BF16),
                pltpu.VMEM((3, 320, 896), BF16),
                pltpu.VMEM((320, 320), F32),
                pltpu.VMEM((320, 80), F32),
                pltpu.VMEM((32, 256), F32),
                pltpu.VMEM((1, 256), F32),
                pltpu.VMEM((16, 1, 256), F32),
                pltpu.VMEM((1, 256), F32),
                pltpu.VMEM((4, 1, 256), F32),
                pltpu.VMEM((2, 2, 4, 56, 128), F32),
                pltpu.VMEM((2, 4, 56, 128), F32),
                pltpu.VMEM((2, 4, 56, 128), F32),
                pltpu.VMEM((4, 2, 56, 128), F32),
                dma((20,)), dma(()),
                dma((2, 16)), dma((2, 16)),
                dma((4, 2)), dma((4,)),
                dma((4, 3)), dma((4, 4)),
                dma((16,)), dma((16,)),
                dma((3,)), dma((4,)),
                dma((2,)), dma((8,)), dma((4, 2)),
            ],
            compiler_params=pltpu.CompilerParams(collective_id=0, has_side_effects=True, vmem_limit_bytes=67043328),
        )(jnp.transpose(ints_blk, (1, 2, 0)), metric_blk, jnp.transpose(orbitals[0]))

    return jax.shard_map(local_fock, mesh=mesh, in_specs=(P(('sys', 'aux'), 'orb', None), P(('sys', 'aux'), None), P('sys', None, None)), out_specs=P('sys', 'orb', 'aux'), check_vma=False)
```

```python
import functools

import jax
import jax.numpy as jnp
from jax import lax
from jax.experimental import pallas as pl
from jax.experimental.pallas import tpu as pltpu
from jax.sharding import PartitionSpec as P

F32, BF16 = jnp.float32, jnp.bfloat16
MESH = pl.DeviceIdType.MESH
NT = (((1,), (1,)), ((), ()))
AHEAD = 8


def split3(x):
    h0 = x.astype(BF16)
    r1 = x - h0.astype(F32)
    h1 = r1.astype(BF16)
    r2 = r1 - h1.astype(F32)
    return h0, h1, r2.astype(BF16)


def dot(a, b):
    return jnp.dot(a, b, preferred_element_type=F32)


def dot_nt(a, b):
    return lax.dot_general(a, b, NT, preferred_element_type=F32)


def kernel(b_hbm, m_hbm, c_ref, out_ref, bb, stage, sbuf, rbuf, mall, mown, cb, c3, tt, ks, kx, jacc, gam, gsend, grecv,
           fsend, frecv, gs, gp, gf, gr, b_sem, m_sem, s_send, s_recv, mz_send, mz_recv, mf_send, mf_recv, g_send, g_recv,
           f_send, f_recv, p_sems, r_send, r_recv):
    a, o = lax.axis_index('aux'), lax.axis_index('orb')
    me = a * 4 + o
    core, row_y = o % 2, o // 2
    core_mate, y_mate = o + 1 - 2 * core, (o + 2) % 4
    planes = [(a + 2) % 4, 3 - a, a + 1 - 2 * (a % 2), a]
    peers = [(planes[k // 4], (o + k % 4) % 4) for k in range(16) if k != 12]

    def remote(src, dst, send, recv, dest):
        return pltpu.make_async_remote_copy(src_ref=src, dst_ref=dst, send_sem=send, recv_sem=recv,
                                            device_id={'aux': dest[0], 'orb': dest[1]}, device_id_type=MESH)

    def b_copy(g):
        rows = pl.ds(g * 4, 4)
        return pltpu.make_async_copy(b_hbm.at[rows], bb.at[rows], b_sem.at[g])

    m_copy = pltpu.make_async_copy(m_hbm, mown, m_sem)
    m_copy.start()
    for g in range(AHEAD):
        b_copy(g).start()

    barrier = pltpu.get_barrier_semaphore()
    for dest in peers:
        pl.semaphore_signal(barrier, inc=1, device_id={'aux': dest[0], 'orb': dest[1]}, device_id_type=MESH)

    m_copy.wait()
    m0, m1, m2 = split3(mown[...])
    pad = jnp.zeros((32, 896), BF16)
    mall[pl.ds(a, 1), 0:224, :] = m0[None]
    mall[pl.ds(a, 1), 224:256, :] = pad[None]
    mall[4, 0:224, :] = m1
    mall[4, 224:256, :] = pad
    mall[5, 0:224, :] = m2
    mall[5, 224:256, :] = pad

    pl.semaphore_wait(barrier, 15)

    quarter = pl.ds(pl.multiple_of(o * 64, 64), 64)

    def mz_copy(plane, step):
        part = mall.at[plane, quarter, :]
        return remote(part, part, mz_send.at[plane, (step + 1) // 2], mz_recv.at[plane], (a + step, o))

    def mf_copy(plane, part_of, dest, k):
        part = mall.at[plane, pl.ds(pl.multiple_of(part_of * 64, 64), 64), :]
        return remote(part, part, mf_send.at[plane, k], mf_recv.at[plane, part_of], (a, dest))

    def relay(r, action):
        for step in (1, -1):
            plane = a - step * r

            @pl.when((plane >= 0) & (plane <= 3))
            def _():
                if action == 'send' and r > 0:
                    mz_copy(plane, step).wait_recv()
                if r < 3:
                    @pl.when((a + step >= 0) & (a + step <= 3))
                    def _():
                        cp = mz_copy(plane, step)
                        cp.start() if action == 'send' else cp.wait_send()
                if action == 'send' and r > 0:
                    mf_copy(plane, o, core_mate, 0).start()
                    mf_copy(plane, o, y_mate, 1).start()

    def pass_on(r):
        for step in (1, -1):
            plane = a - step * r

            @pl.when((plane >= 0) & (plane <= 3))
            def _():
                mf_copy(plane, y_mate, y_mate, 2).wait_recv()
                mf_copy(plane, y_mate, core_mate, 2).start()

    relay(0, 'send')

    def half_copy(ii, dest, rows):
        d = dest[0] * 4 + dest[1]
        return remote(sbuf.at[2 * d + ii, rows, :], rbuf.at[ii, me, rows, :], s_send.at[ii, d], s_recv.at[ii, me], dest)

    parts = split3(c_ref[...])
    zero = jnp.zeros((32, 320), BF16)
    for k in range(3):
        rows = [parts[k] if j <= 2 - k else zero for j in range(3)]
        c3[32 * k:32 * k + 32, :] = jnp.concatenate(rows + [zero[:, :64]], axis=1)
    own = jnp.zeros((32, 80), F32)
    for k in range(4):
        own = jnp.where(o == k, c_ref[:, 80 * k:80 * k + 80], own)
    for m in range(80):
        cb[m] = jnp.broadcast_to(own[:, m:m + 1], (32, 128))
    stage[1] = jnp.zeros((512, 128), F32)
    gam[...] = jnp.zeros((32, 256), F32)

    def group(g, carry):
        for k in range(2):
            b_copy(2 * g + k).wait()

        @pl.when(2 * g + AHEAD < 20)
        def _():
            for k in range(2):
                b_copy(2 * g + k + AHEAD).start()

        base = lax.rem(g, 2) * 8

        def rows4(k, carry):
            part0 = part1 = None
            for j in range(4):
                m = 4 * k + j
                w = jnp.concatenate(list(split3(bb[g * 8 + m])) + [jnp.zeros((64, 224), BF16)], axis=0)
                r = dot(c3[...], w)
                h = r[0:32] + r[32:64] + r[64:96]
                stage[0, pl.ds(base + m, 32, stride=16), :] = h[:, :128]
                stage[1, pl.ds(base + m, 32, stride=16), 0:96] = h[:, 128:]
                coef = cb[g * 8 + m]
                add0, add1 = h[:, :128] * coef, h[:, 128:] * coef[:, :96]
                part0 = add0 if part0 is None else part0 + add0
                part1 = add1 if part1 is None else part1 + add1
            gam[:, 0:128] += part0
            gam[:, 128:224] += part1
            return carry

        lax.fori_loop(0, 2, rows4, 0)

        @pl.when(lax.rem(g, 2) == 1)
        def _():
            rows = pl.ds(pl.multiple_of((g // 2) * 16, 16), 16)
            for t in range(2):
                sbuf[:, rows, 128 * t:128 * t + 128] = stage[t].reshape(32, 16, 128).astype(BF16)
            for dest in peers:
                half_copy(0, dest, rows).start()

        @pl.when(g == 1)
        def _():
            relay(1, 'send')

        @pl.when(g == 4)
        def _():
            relay(2, 'send')
            pass_on(1)

        return carry

    lax.fori_loop(0, 10, group, 0)

    def g_copy(dest):
        return remote(gsend, grecv.at[me], g_send.at[dest[0] * 4 + dest[1]], g_recv.at[me], dest)

    g_row = jnp.sum(gam[...], axis=0, keepdims=True)
    gsend[...] = g_row
    grecv[pl.ds(me, 1)] = g_row[None]
    for dest in peers:
        g_copy(dest).start()

    full = pl.ds(0, 80)
    for dest in peers:
        half_copy(1, dest, pl.ds(0, 48)).start()
    rbuf[:, pl.ds(me, 1)] = sbuf[pl.ds(2 * me, 2)][:, None]
    relay(3, 'send')
    pass_on(2)

    def lanes_of(rows):
        return jnp.concatenate([r[:, :224] for r in rows], axis=1)

    def as_row(col):
        x = jnp.broadcast_to(col, (224, 128))
        return jnp.concatenate([jnp.transpose(x[:128])[0:1], jnp.transpose(x[96:])[0:1, 32:], jnp.zeros((1, 32), F32)],
                               axis=1)

    def times_metric(row):
        return jnp.sum(mown[...] * row, axis=1, keepdims=True)

    for s in peers:
        remote(gsend, grecv.at[s[0] * 4 + s[1]], g_send.at[0], g_recv.at[s[0] * 4 + s[1]], s).wait_recv()
    gamma = lanes_of([grecv[4 * b] + grecv[4 * b + 1] + grecv[4 * b + 2] + grecv[4 * b + 3] for b in range(4)])
    fit_row = as_row(times_metric(gamma))
    fsend[...] = fit_row
    frecv[pl.ds(a, 1)] = fit_row[None]

    def f_copy(j):
        return remote(fsend, frecv.at[a], f_send.at[j], f_recv.at[a], (planes[j], o))

    for j in range(3):
        f_copy(j).start()
    for dest in peers:
        half_copy(1, dest, pl.ds(48, 32)).start()
    pass_on(3)

    for r in range(1, 4):
        for step in (1, -1):
            plane = a - step * r

            @pl.when((plane >= 0) & (plane <= 3))
            def _():
                for part_of in (core_mate, 3 - o):
                    mf_copy(plane, part_of, part_of, 0).wait_recv()

    def t_and_k(ii):
        for s in peers:
            n = s[0] * 4 + s[1]
            remote(sbuf.at[ii], rbuf.at[ii, n], s_send.at[ii, n], s_recv.at[ii, n], s).wait_recv()
        for n0, n1 in ((0, 256), (256, 512), (512, 768), (768, 896)):
            t = dot(rbuf[ii, 0:4].reshape(320, 256), mall[0, :, n0:n1])
            for b in range(1, 4):
                t += dot(rbuf[ii, 4 * b:4 * b + 4].reshape(320, 256), mall[b, :, n0:n1])
            mine = rbuf[ii, pl.ds(a * 4, 4)].reshape(320, 256)
            t += dot(mine, mall[4, :, n0:n1]) + dot(mine, mall[5, :, n0:n1])
            for k, h in enumerate(split3(t)):
                tt[k, :, n0:n1] = h
        t0, t1, t2 = tt[0], tt[1], tt[2]
        same = dot_nt(t0, t0) + dot_nt(t1, t1)
        cross = dot_nt(t0, t1) + dot_nt(t0, t2)
        if ii == 0:
            ks[...] = same
            kx[...] = cross
        else:
            cross = kx[...] + cross
            ks[...] += same + cross + jnp.transpose(cross)

    t_and_k(0)
    for j in range(3):
        remote(fsend, frecv.at[planes[j]], f_send.at[j], f_recv.at[planes[j]], (planes[j], o)).wait_recv()
    weights = times_metric(lanes_of([frecv[b] for b in range(4)]))
    w_row = as_row(2.0 * weights)

    lane = lax.broadcasted_iota(jnp.int32, (8, 128), 1)
    w0, w1 = jnp.broadcast_to(w_row[:, :128], (8, 128)), jnp.broadcast_to(w_row[:, 128:224], (8, 96))

    zero32 = jnp.zeros((8, 32), F32)

    def coul(k, carry):
        rows = pl.ds(pl.multiple_of(k * 8, 8), 8)
        acc = jnp.zeros((8, 128), F32)
        for m in range(80):
            z = jnp.concatenate([bb[m, rows, 128:224] * w1, zero32], axis=1)
            col = jnp.sum(bb[m, rows, 0:128] * w0 + z, axis=1, keepdims=True)
            acc = jnp.where(lane == m, col, acc)
        jacc[rows, :] = acc[:, :80]
        return carry

    lax.fori_loop(0, 40, coul, 0)
    jt = jnp.transpose(jacc[...])

    t_and_k(1)

    def packed(x):
        tail = jnp.concatenate([x[56:, :48], jnp.concatenate([x[56:, 48:], jnp.zeros((24, 16), F32)], axis=1),
                                jnp.zeros((8, 48), F32)], axis=0)
        return jnp.concatenate([x[:56], tail], axis=1)

    for c in range(4):
        for k in range(4):
            gs[k % 2, k // 2, c] = packed(jnp.where(o == k, jt[:, 80 * c:80 * c + 80], 0.0)
                                          - ks[80 * k:80 * k + 80, 80 * c:80 * c + 80])
    pair = remote(gs.at[1 - core], gp, p_sems.at[0], p_sems.at[1], (a, core_mate))
    pair.start()
    pair.wait()
    gf[...] = gs[core] + gp[...]

    def r_copy(k):
        plane, y = planes[k // 2], (row_y + k % 2) % 2
        return remote(gf.at[y, plane], gr.at[a, row_y], r_send.at[k], r_recv.at[a, row_y], (plane, 2 * y + core))

    r_order = (0, 1, 2, 3, 4, 5, 7)
    for k in r_order:
        r_copy(k).start()
    total = gf[row_y, a]
    for k in r_order:
        plane, y = planes[k // 2], (row_y + k % 2) % 2
        remote(gf.at[y, plane], gr.at[plane, y], r_send.at[k], r_recv.at[plane, y], (plane, 2 * y + core)).wait_recv()
        total = total + gr[plane, y]
    out_ref[0] = jnp.concatenate([total[:, :80], jnp.concatenate([total[0:24, 80:128], total[24:48, 80:112]], axis=1)], axis=0)


    for dest in peers:
        half_copy(0, dest, full).wait_send()
        half_copy(1, dest, full).wait_send()
        g_copy(dest).wait_send()
    for k in r_order:
        r_copy(k).wait_send()
    for r in range(3):
        relay(r, 'drain')
    for j in range(3):
        f_copy(j).wait_send()
        for k in range(3):
            mf_copy(planes[j], o, o, k).wait_send()


def solution(mesh):
    def local_fock(ints_blk, metric_blk, orbitals):
        dma = pltpu.SemaphoreType.DMA
        return pl.pallas_call(
            kernel,
            name='fock',
            out_shape=jax.ShapeDtypeStruct((1, 80, 80), F32),
            in_specs=[pl.BlockSpec(memory_space=pl.ANY), pl.BlockSpec(memory_space=pl.ANY),
                      pl.BlockSpec(memory_space=pltpu.VMEM)],
            out_specs=pl.BlockSpec(memory_space=pltpu.VMEM),
            scratch_shapes=[
                pltpu.VMEM((80, 320, 224), F32),
                pltpu.VMEM((2, 512, 128), F32),
                pltpu.VMEM((32, 80, 256), BF16),
                pltpu.VMEM((2, 16, 80, 256), BF16),
                pltpu.VMEM((6, 256, 896), BF16),
                pltpu.VMEM((224, 896), F32),
                pltpu.VMEM((80, 32, 128), F32),
                pltpu.VMEM((96, 1024), BF16),
                pltpu.VMEM((3, 320, 896), BF16),
                pltpu.VMEM((320, 320), F32),
                pltpu.VMEM((320, 320), F32),
                pltpu.VMEM((320, 80), F32),
                pltpu.VMEM((32, 256), F32),
                pltpu.VMEM((1, 256), F32),
                pltpu.VMEM((16, 1, 256), F32),
                pltpu.VMEM((1, 256), F32),
                pltpu.VMEM((4, 1, 256), F32),
                pltpu.VMEM((2, 2, 4, 56, 128), F32),
                pltpu.VMEM((2, 4, 56, 128), F32),
                pltpu.VMEM((2, 4, 56, 128), F32),
                pltpu.VMEM((4, 2, 56, 128), F32),
                dma((20,)), dma(()),
                dma((2, 16)), dma((2, 16)),
                dma((4, 2)), dma((4,)),
                dma((4, 3)), dma((4, 4)),
                dma((16,)), dma((16,)),
                dma((3,)), dma((4,)),
                dma((2,)), dma((8,)), dma((4, 2)),
            ],
            compiler_params=pltpu.CompilerParams(collective_id=0, has_side_effects=True, vmem_limit_bytes=67043328),
        )(jnp.transpose(ints_blk, (1, 2, 0)), metric_blk, jnp.transpose(orbitals[0]))

    return jax.shard_map(local_fock, mesh=mesh, in_specs=(P(('sys', 'aux'), 'orb', None), P(('sys', 'aux'), None), P('sys', None, None)), out_specs=P('sys', 'orb', 'aux'), check_vma=False)
```

```python
import functools

import jax
import jax.numpy as jnp
from jax import lax
from jax.experimental import pallas as pl
from jax.experimental.pallas import tpu as pltpu
from jax.sharding import PartitionSpec as P

F32, BF16 = jnp.float32, jnp.bfloat16
MESH = pl.DeviceIdType.MESH
NT = (((1,), (1,)), ((), ()))
AHEAD = 8


def split3(x):
    h0 = x.astype(BF16)
    r1 = x - h0.astype(F32)
    h1 = r1.astype(BF16)
    r2 = r1 - h1.astype(F32)
    return h0, h1, r2.astype(BF16)


def dot(a, b):
    return jnp.dot(a, b, preferred_element_type=F32)


def dot_nt(a, b):
    return lax.dot_general(a, b, NT, preferred_element_type=F32)


def kernel(b_hbm, m_hbm, c_ref, out_ref, bb, stage, sbuf, rbuf, mall, mown, cb, c3, tt, ks, kx, jacc, gam, gsend, grecv,
           fsend, frecv, gs, gp, gf, gr, b_sem, m_sem, s_send, s_recv, mz_send, mz_recv, mf_send, mf_recv, g_send, g_recv,
           f_send, f_recv, p_sems, r_send, r_recv):
    a, o = lax.axis_index('aux'), lax.axis_index('orb')
    me = a * 4 + o
    core, row_y = o % 2, o // 2
    core_mate, y_mate = o + 1 - 2 * core, (o + 2) % 4
    planes = [(a + 2) % 4, 3 - a, a + 1 - 2 * (a % 2), a]
    peers = [(planes[k // 4], (o + k % 4) % 4) for k in range(16) if k != 12]

    def remote(src, dst, send, recv, dest):
        return pltpu.make_async_remote_copy(src_ref=src, dst_ref=dst, send_sem=send, recv_sem=recv,
                                            device_id={'aux': dest[0], 'orb': dest[1]}, device_id_type=MESH)

    def b_copy(g):
        rows = pl.ds(g * 4, 4)
        return pltpu.make_async_copy(b_hbm.at[rows], bb.at[rows], b_sem.at[g])

    m_copy = pltpu.make_async_copy(m_hbm, mown, m_sem)
    m_copy.start()
    for g in range(2):
        b_copy(g).start()

    barrier = pltpu.get_barrier_semaphore()
    for dest in peers:
        pl.semaphore_signal(barrier, inc=1, device_id={'aux': dest[0], 'orb': dest[1]}, device_id_type=MESH)

    m_copy.wait()
    for g in range(2, AHEAD):
        b_copy(g).start()
    m0, m1, m2 = split3(mown[...])
    pad = jnp.zeros((32, 896), BF16)
    mall[pl.ds(a, 1), 0:224, :] = m0[None]
    mall[pl.ds(a, 1), 224:256, :] = pad[None]
    mall[4, 0:224, :] = m1
    mall[4, 224:256, :] = pad
    mall[5, 0:224, :] = m2
    mall[5, 224:256, :] = pad

    pl.semaphore_wait(barrier, 15)

    quarter = pl.ds(pl.multiple_of(o * 64, 64), 64)

    def mz_copy(plane, step):
        part = mall.at[plane, quarter, :]
        return remote(part, part, mz_send.at[plane, (step + 1) // 2], mz_recv.at[plane], (a + step, o))

    def mf_copy(plane, part_of, dest, k):
        part = mall.at[plane, pl.ds(pl.multiple_of(part_of * 64, 64), 64), :]
        return remote(part, part, mf_send.at[plane, k], mf_recv.at[plane, part_of], (a, dest))

    def relay(r, action):
        for step in (1, -1):
            plane = a - step * r

            @pl.when((plane >= 0) & (plane <= 3))
            def _():
                if action == 'send' and r > 0:
                    mz_copy(plane, step).wait_recv()
                if r < 3:
                    @pl.when((a + step >= 0) & (a + step <= 3))
                    def _():
                        cp = mz_copy(plane, step)
                        cp.start() if action == 'send' else cp.wait_send()
                if action == 'send' and r > 0:
                    mf_copy(plane, o, core_mate, 0).start()
                    mf_copy(plane, o, y_mate, 1).start()

    def pass_on(r):
        for step in (1, -1):
            plane = a - step * r

            @pl.when((plane >= 0) & (plane <= 3))
            def _():
                mf_copy(plane, y_mate, y_mate, 2).wait_recv()
                mf_copy(plane, y_mate, core_mate, 2).start()

    relay(0, 'send')

    def half_copy(ii, dest, rows):
        d = dest[0] * 4 + dest[1]
        return remote(sbuf.at[2 * d + ii, rows, :], rbuf.at[ii, me, rows, :], s_send.at[ii, d], s_recv.at[ii, me], dest)

    parts = split3(c_ref[...])
    zero = jnp.zeros((32, 320), BF16)
    for k in range(3):
        rows = [parts[k] if j <= 2 - k else zero for j in range(3)]
        c3[32 * k:32 * k + 32, :] = jnp.concatenate(rows + [zero[:, :64]], axis=1)
    own = jnp.zeros((32, 80), F32)
    for k in range(4):
        own = jnp.where(o == k, c_ref[:, 80 * k:80 * k + 80], own)
    for m in range(80):
        cb[m] = jnp.broadcast_to(own[:, m:m + 1], (32, 128))
    stage[1] = jnp.zeros((512, 128), F32)
    gam[...] = jnp.zeros((32, 256), F32)

    def group(g, carry):
        for k in range(2):
            b_copy(2 * g + k).wait()

        @pl.when(2 * g + AHEAD < 20)
        def _():
            for k in range(2):
                b_copy(2 * g + k + AHEAD).start()

        base = lax.rem(g, 2) * 8

        def rows4(k, carry):
            part0 = part1 = None
            for j in range(4):
                m = 4 * k + j
                w = jnp.concatenate(list(split3(bb[g * 8 + m])) + [jnp.zeros((64, 224), BF16)], axis=0)
                r = dot(c3[...], w)
                h = r[0:32] + r[32:64] + r[64:96]
                stage[0, pl.ds(base + m, 32, stride=16), :] = h[:, :128]
                stage[1, pl.ds(base + m, 32, stride=16), 0:96] = h[:, 128:]
                coef = cb[g * 8 + m]
                add0, add1 = h[:, :128] * coef, h[:, 128:] * coef[:, :96]
                part0 = add0 if part0 is None else part0 + add0
                part1 = add1 if part1 is None else part1 + add1
            gam[:, 0:128] += part0
            gam[:, 128:224] += part1
            return carry

        lax.fori_loop(0, 2, rows4, 0)

        @pl.when(lax.rem(g, 2) == 1)
        def _():
            rows = pl.ds(pl.multiple_of((g // 2) * 16, 16), 16)
            for t in range(2):
                sbuf[:, rows, 128 * t:128 * t + 128] = stage[t].reshape(32, 16, 128).astype(BF16)
            for dest in peers:
                half_copy(0, dest, rows).start()

        @pl.when(g == 5)
        def _():
            relay(1, 'send')

        return carry

    lax.fori_loop(0, 10, group, 0)
    relay(2, 'send')
    pass_on(1)

    def g_copy(dest):
        return remote(gsend, grecv.at[me], g_send.at[dest[0] * 4 + dest[1]], g_recv.at[me], dest)

    g_row = jnp.sum(gam[...], axis=0, keepdims=True)
    gsend[...] = g_row
    grecv[pl.ds(me, 1)] = g_row[None]
    for dest in peers:
        g_copy(dest).start()

    full = pl.ds(0, 80)
    for dest in peers:
        half_copy(1, dest, pl.ds(0, 16)).start()
    rbuf[:, pl.ds(me, 1)] = sbuf[pl.ds(2 * me, 2)][:, None]
    relay(3, 'send')
    pass_on(2)

    def lanes_of(rows):
        return jnp.concatenate([r[:, :224] for r in rows], axis=1)

    def as_row(col):
        x = jnp.broadcast_to(col, (224, 128))
        return jnp.concatenate([jnp.transpose(x[:128])[0:1], jnp.transpose(x[96:])[0:1, 32:], jnp.zeros((1, 32), F32)],
                               axis=1)

    def times_metric(row):
        return jnp.sum(mown[...] * row, axis=1, keepdims=True)

    for s in peers:
        remote(gsend, grecv.at[s[0] * 4 + s[1]], g_send.at[0], g_recv.at[s[0] * 4 + s[1]], s).wait_recv()
    gamma = lanes_of([grecv[4 * b] + grecv[4 * b + 1] + grecv[4 * b + 2] + grecv[4 * b + 3] for b in range(4)])
    fit_row = as_row(times_metric(gamma))
    fsend[...] = fit_row
    frecv[pl.ds(a, 1)] = fit_row[None]

    def f_copy(j):
        return remote(fsend, frecv.at[a], f_send.at[j], f_recv.at[a], (planes[j], o))

    for j in range(3):
        f_copy(j).start()
    for dest in peers:
        half_copy(1, dest, pl.ds(16, 64)).start()
    pass_on(3)

    for r in range(1, 4):
        for step in (1, -1):
            plane = a - step * r

            @pl.when((plane >= 0) & (plane <= 3))
            def _():
                for part_of in (core_mate, 3 - o):
                    mf_copy(plane, part_of, part_of, 0).wait_recv()

    def t_and_k(ii):
        for s in peers:
            n = s[0] * 4 + s[1]
            remote(sbuf.at[ii], rbuf.at[ii, n], s_send.at[ii, n], s_recv.at[ii, n], s).wait_recv()
        for n0, n1 in ((0, 256), (256, 512), (512, 768), (768, 896)):
            t = dot(rbuf[ii, 0:4].reshape(320, 256), mall[0, :, n0:n1])
            for b in range(1, 4):
                t += dot(rbuf[ii, 4 * b:4 * b + 4].reshape(320, 256), mall[b, :, n0:n1])
            mine = rbuf[ii, pl.ds(a * 4, 4)].reshape(320, 256)
            t += dot(mine, mall[4, :, n0:n1]) + dot(mine, mall[5, :, n0:n1])
            for k, h in enumerate(split3(t)):
                tt[k, :, n0:n1] = h
        t0, t1, t2 = tt[0], tt[1], tt[2]
        same = dot_nt(t0, t0) + dot_nt(t1, t1)
        cross = dot_nt(t0, t1) + dot_nt(t0, t2)
        if ii == 0:
            ks[...] = same
            kx[...] = cross
        else:
            cross = kx[...] + cross
            ks[...] += same + cross + jnp.transpose(cross)

    t_and_k(0)
    for j in range(3):
        remote(fsend, frecv.at[planes[j]], f_send.at[j], f_recv.at[planes[j]], (planes[j], o)).wait_recv()
    weights = times_metric(lanes_of([frecv[b] for b in range(4)]))
    w_row = as_row(2.0 * weights)

    lane = lax.broadcasted_iota(jnp.int32, (8, 128), 1)
    w0, w1 = jnp.broadcast_to(w_row[:, :128], (8, 128)), jnp.broadcast_to(w_row[:, 128:224], (8, 96))

    zero32 = jnp.zeros((8, 32), F32)

    def coul(k, carry):
        for j in range(4):
            rows = pl.ds(pl.multiple_of(k * 32 + 8 * j, 8), 8)
            acc = jnp.zeros((8, 128), F32)
            for m in range(80):
                z = jnp.concatenate([bb[m, rows, 128:224] * w1, zero32], axis=1)
                col = jnp.sum(bb[m, rows, 0:128] * w0 + z, axis=1, keepdims=True)
                acc = jnp.where(lane == m, col, acc)
            jacc[rows, :] = acc[:, :80]
        return carry

    lax.fori_loop(0, 10, coul, 0)
    jt = jnp.transpose(jacc[...])

    t_and_k(1)

    def packed(x):
        tail = jnp.concatenate([x[56:, :48], jnp.concatenate([x[56:, 48:], jnp.zeros((24, 16), F32)], axis=1),
                                jnp.zeros((8, 48), F32)], axis=0)
        return jnp.concatenate([x[:56], tail], axis=1)

    for c in range(4):
        for k in range(4):
            gs[k % 2, k // 2, c] = packed(jnp.where(o == k, jt[:, 80 * c:80 * c + 80], 0.0)
                                          - ks[80 * k:80 * k + 80, 80 * c:80 * c + 80])
    pair = remote(gs.at[1 - core], gp, p_sems.at[0], p_sems.at[1], (a, core_mate))
    pair.start()
    pair.wait()
    gf[...] = gs[core] + gp[...]

    def r_copy(k):
        plane, y = planes[k // 2], (row_y + k % 2) % 2
        return remote(gf.at[y, plane], gr.at[a, row_y], r_send.at[k], r_recv.at[a, row_y], (plane, 2 * y + core))

    r_order = (0, 1, 2, 3, 4, 5, 7)
    for k in r_order:
        r_copy(k).start()
    total = gf[row_y, a]
    for k in r_order:
        plane, y = planes[k // 2], (row_y + k % 2) % 2
        remote(gf.at[y, plane], gr.at[plane, y], r_send.at[k], r_recv.at[plane, y], (plane, 2 * y + core)).wait_recv()
        total = total + gr[plane, y]
    out_ref[0] = jnp.concatenate([total[:, :80], jnp.concatenate([total[0:24, 80:128], total[24:48, 80:112]], axis=1)], axis=0)


    for dest in peers:
        half_copy(0, dest, full).wait_send()
        half_copy(1, dest, full).wait_send()
        g_copy(dest).wait_send()
    for k in r_order:
        r_copy(k).wait_send()
    for r in range(3):
        relay(r, 'drain')
    for j in range(3):
        f_copy(j).wait_send()
        for k in range(3):
            mf_copy(planes[j], o, o, k).wait_send()


def solution(mesh):
    def local_fock(ints_blk, metric_blk, orbitals):
        dma = pltpu.SemaphoreType.DMA
        return pl.pallas_call(
            kernel,
            name='fock',
            out_shape=jax.ShapeDtypeStruct((1, 80, 80), F32),
            in_specs=[pl.BlockSpec(memory_space=pl.ANY), pl.BlockSpec(memory_space=pl.ANY),
                      pl.BlockSpec(memory_space=pltpu.VMEM)],
            out_specs=pl.BlockSpec(memory_space=pltpu.VMEM),
            scratch_shapes=[
                pltpu.VMEM((80, 320, 224), F32),
                pltpu.VMEM((2, 512, 128), F32),
                pltpu.VMEM((32, 80, 256), BF16),
                pltpu.VMEM((2, 16, 80, 256), BF16),
                pltpu.VMEM((6, 256, 896), BF16),
                pltpu.VMEM((224, 896), F32),
                pltpu.VMEM((80, 32, 128), F32),
                pltpu.VMEM((96, 1024), BF16),
                pltpu.VMEM((3, 320, 896), BF16),
                pltpu.VMEM((320, 320), F32),
                pltpu.VMEM((320, 320), F32),
                pltpu.VMEM((320, 80), F32),
                pltpu.VMEM((32, 256), F32),
                pltpu.VMEM((1, 256), F32),
                pltpu.VMEM((16, 1, 256), F32),
                pltpu.VMEM((1, 256), F32),
                pltpu.VMEM((4, 1, 256), F32),
                pltpu.VMEM((2, 2, 4, 56, 128), F32),
                pltpu.VMEM((2, 4, 56, 128), F32),
                pltpu.VMEM((2, 4, 56, 128), F32),
                pltpu.VMEM((4, 2, 56, 128), F32),
                dma((20,)), dma(()),
                dma((2, 16)), dma((2, 16)),
                dma((4, 2)), dma((4,)),
                dma((4, 3)), dma((4, 4)),
                dma((16,)), dma((16,)),
                dma((3,)), dma((4,)),
                dma((2,)), dma((8,)), dma((4, 2)),
            ],
            compiler_params=pltpu.CompilerParams(collective_id=0, has_side_effects=True, vmem_limit_bytes=67043328),
        )(jnp.transpose(ints_blk, (1, 2, 0)), metric_blk, jnp.transpose(orbitals[0]))

    return jax.shard_map(local_fock, mesh=mesh, in_specs=(P(('sys', 'aux'), 'orb', None), P(('sys', 'aux'), None), P('sys', None, None)), out_specs=P('sys', 'orb', 'aux'), check_vma=False)
```

```python
import functools

import jax
import jax.numpy as jnp
from jax import lax
from jax.experimental import pallas as pl
from jax.experimental.pallas import tpu as pltpu
from jax.sharding import PartitionSpec as P

F32, BF16 = jnp.float32, jnp.bfloat16
MESH = pl.DeviceIdType.MESH
NT = (((1,), (1,)), ((), ()))
AHEAD = 8


def split3(x):
    h0 = x.astype(BF16)
    r1 = x - h0.astype(F32)
    h1 = r1.astype(BF16)
    r2 = r1 - h1.astype(F32)
    return h0, h1, r2.astype(BF16)


def dot(a, b):
    return jnp.dot(a, b, preferred_element_type=F32)


def dot_nt(a, b):
    return lax.dot_general(a, b, NT, preferred_element_type=F32)


def kernel(b_hbm, m_hbm, c_ref, out_ref, bb, stage, smain, srest, rmain, rrest, rest, mall, mown, cb, c3, tt, ks, kx, jacc, gam, gsend, grecv,
           fsend, frecv, gs, gp, gf, gr, b_sem, m_sem, s_send, s_recv, mz_send, mz_recv, mf_send, mf_recv, g_send, g_recv,
           f_send, f_recv, p_sems, r_send, r_recv):
    a, o = lax.axis_index('aux'), lax.axis_index('orb')
    me = a * 4 + o
    core, row_y = o % 2, o // 2
    core_mate, y_mate = o + 1 - 2 * core, (o + 2) % 4
    planes = [(a + 2) % 4, 3 - a, a + 1 - 2 * (a % 2), a]
    peers = [(planes[k // 4], (o + k % 4) % 4) for k in range(16) if k != 12]

    def remote(src, dst, send, recv, dest):
        return pltpu.make_async_remote_copy(src_ref=src, dst_ref=dst, send_sem=send, recv_sem=recv,
                                            device_id={'aux': dest[0], 'orb': dest[1]}, device_id_type=MESH)

    def b_copy(g):
        rows = pl.ds(g * 4, 4)
        return pltpu.make_async_copy(b_hbm.at[rows], bb.at[rows], b_sem.at[g])

    m_copy = pltpu.make_async_copy(m_hbm, mown, m_sem)
    m_copy.start()
    for g in range(2):
        b_copy(g).start()

    barrier = pltpu.get_barrier_semaphore()
    for dest in peers:
        pl.semaphore_signal(barrier, inc=1, device_id={'aux': dest[0], 'orb': dest[1]}, device_id_type=MESH)

    m_copy.wait()
    for g in range(2, AHEAD):
        b_copy(g).start()
    m0, m1, m2 = split3(mown[...])
    pad = jnp.zeros((32, 896), BF16)
    mall[pl.ds(a, 1), 0:224, :] = m0[None]
    mall[pl.ds(a, 1), 224:256, :] = pad[None]
    mall[4, 0:224, :] = m1
    mall[4, 224:256, :] = pad
    mall[5, 0:224, :] = m2
    mall[5, 224:256, :] = pad

    pl.semaphore_wait(barrier, 15)

    quarter = pl.ds(pl.multiple_of(o * 64, 64), 64)

    def mz_copy(plane, step):
        part = mall.at[plane, quarter, :]
        return remote(part, part, mz_send.at[plane, (step + 1) // 2], mz_recv.at[plane], (a + step, o))

    def mf_copy(plane, part_of, dest, k):
        part = mall.at[plane, pl.ds(pl.multiple_of(part_of * 64, 64), 64), :]
        return remote(part, part, mf_send.at[plane, k], mf_recv.at[plane, part_of], (a, dest))

    def relay(r, action):
        for step in (1, -1):
            plane = a - step * r

            @pl.when((plane >= 0) & (plane <= 3))
            def _():
                if action == 'send' and r > 0:
                    mz_copy(plane, step).wait_recv()
                if r < 3:
                    @pl.when((a + step >= 0) & (a + step <= 3))
                    def _():
                        cp = mz_copy(plane, step)
                        cp.start() if action == 'send' else cp.wait_send()
                if action == 'send' and r > 0:
                    mf_copy(plane, o, core_mate, 0).start()
                    mf_copy(plane, o, y_mate, 1).start()

    def pass_on(r):
        for step in (1, -1):
            plane = a - step * r

            @pl.when((plane >= 0) & (plane <= 3))
            def _():
                mf_copy(plane, y_mate, y_mate, 2).wait_recv()
                mf_copy(plane, y_mate, core_mate, 2).start()

    relay(0, 'send')

    def main_copy(dest, rows):
        d = dest[0] * 4 + dest[1]
        return remote(smain.at[pl.ds(2 * d, 2), rows, :], rmain.at[:, me, rows, :], s_send.at[2, d], s_recv.at[2, me], dest)

    def rest_copy(ii, dest):
        d = dest[0] * 4 + dest[1]
        return remote(srest.at[2 * d + ii], rrest.at[ii, me], s_send.at[ii, d], s_recv.at[ii, me], dest)

    parts = split3(c_ref[...])
    zero = jnp.zeros((32, 320), BF16)
    for k in range(3):
        rows = [parts[k] if j <= 2 - k else zero for j in range(3)]
        c3[32 * k:32 * k + 32, :] = jnp.concatenate(rows + [zero[:, :64]], axis=1)
    own = jnp.zeros((32, 80), F32)
    for k in range(4):
        own = jnp.where(o == k, c_ref[:, 80 * k:80 * k + 80], own)
    for m in range(80):
        cb[m] = jnp.broadcast_to(own[:, m:m + 1], (32, 128))
    rest[...] = jnp.zeros((16, 80, 128), BF16)
    srest[:, :, 384:512] = jnp.zeros((32, 16, 128), BF16)
    gam[...] = jnp.zeros((32, 256), F32)

    def group(g, carry):
        for k in range(2):
            b_copy(2 * g + k).wait()

        @pl.when(2 * g + AHEAD < 20)
        def _():
            for k in range(2):
                b_copy(2 * g + k + AHEAD).start()

        base = lax.rem(g, 2) * 8

        def rows4(k, carry):
            part0 = part1 = None
            for j in range(4):
                m = 4 * k + j
                w = jnp.concatenate(list(split3(bb[g * 8 + m])) + [jnp.zeros((64, 224), BF16)], axis=0)
                r = dot(c3[...], w)
                h = r[0:32] + r[32:64] + r[64:96]
                stage[0, pl.ds(base + m, 32, stride=16), :] = h[:, :128]
                stage[1, pl.ds(base + m, 32, stride=16), 0:96] = h[:, 128:]
                coef = cb[g * 8 + m]
                add0, add1 = h[:, :128] * coef, h[:, 128:] * coef[:, :96]
                part0 = add0 if part0 is None else part0 + add0
                part1 = add1 if part1 is None else part1 + add1
            gam[:, 0:128] += part0
            gam[:, 128:224] += part1
            return carry

        lax.fori_loop(0, 2, rows4, 0)

        @pl.when(lax.rem(g, 2) == 1)
        def _():
            rows = pl.ds(pl.multiple_of((g // 2) * 16, 16), 16)
            smain[:, rows, :] = stage[0].reshape(32, 16, 128).astype(BF16)
            for dest in peers:
                main_copy(dest, rows).start()

        for c in range(5):
            @pl.when(g == 2 * c + 1)
            def _():
                at = 96 * c if c < 4 else 384
                srest[:, :, at:at + 96] = stage[1].reshape(32, 16, 128)[:, :, :96].astype(BF16)

        @pl.when(g == 5)
        def _():
            relay(1, 'send')

        return carry

    lax.fori_loop(0, 10, group, 0)
    relay(2, 'send')
    pass_on(1)

    def g_copy(dest):
        return remote(gsend, grecv.at[me], g_send.at[dest[0] * 4 + dest[1]], g_recv.at[me], dest)

    g_row = jnp.sum(gam[...], axis=0, keepdims=True)
    gsend[...] = g_row
    grecv[pl.ds(me, 1)] = g_row[None]
    for dest in peers:
        g_copy(dest).start()

    for dest in peers:
        rest_copy(0, dest).start()
    rmain[:, pl.ds(me, 1)] = smain[pl.ds(2 * me, 2)][:, None]
    rrest[:, pl.ds(me, 1)] = srest[pl.ds(2 * me, 2)][:, None]
    relay(3, 'send')
    pass_on(2)

    def lanes_of(rows):
        return jnp.concatenate([r[:, :224] for r in rows], axis=1)

    def as_row(col):
        x = jnp.broadcast_to(col, (224, 128))
        return jnp.concatenate([jnp.transpose(x[:128])[0:1], jnp.transpose(x[96:])[0:1, 32:], jnp.zeros((1, 32), F32)],
                               axis=1)

    def times_metric(row):
        return jnp.sum(mown[...] * row, axis=1, keepdims=True)

    for s in peers:
        remote(gsend, grecv.at[s[0] * 4 + s[1]], g_send.at[0], g_recv.at[s[0] * 4 + s[1]], s).wait_recv()
    gamma = lanes_of([grecv[4 * b] + grecv[4 * b + 1] + grecv[4 * b + 2] + grecv[4 * b + 3] for b in range(4)])
    fit_row = as_row(times_metric(gamma))
    fsend[...] = fit_row
    frecv[pl.ds(a, 1)] = fit_row[None]

    def f_copy(j):
        return remote(fsend, frecv.at[a], f_send.at[j], f_recv.at[a], (planes[j], o))

    for j in range(3):
        f_copy(j).start()
    for dest in peers:
        rest_copy(1, dest).start()
    pass_on(3)

    for r in range(1, 4):
        for step in (1, -1):
            plane = a - step * r

            @pl.when((plane >= 0) & (plane <= 3))
            def _():
                for part_of in (core_mate, 3 - o):
                    mf_copy(plane, part_of, part_of, 0).wait_recv()

    def t_and_k(ii):
        for s in peers:
            n = s[0] * 4 + s[1]
            if ii == 0:
                remote(smain.at[pl.ds(0, 2)], rmain.at[:, n], s_send.at[2, n], s_recv.at[2, n], s).wait_recv()
            remote(srest.at[ii], rrest.at[ii, n], s_send.at[ii, n], s_recv.at[ii, n], s).wait_recv()
        for n in range(16):
            for c in range(5):
                at = 96 * c if c < 4 else 384
                rest[n, 16 * c:16 * c + 16, 0:96] = rrest[ii, n, :, at:at + 96]

        def rows_of(plane):
            four = pl.ds(4 * plane, 4)
            return jnp.concatenate([rmain[ii, four].reshape(320, 128), rest[four].reshape(320, 128)], axis=1)

        for n0, n1 in ((0, 256), (256, 512), (512, 768), (768, 896)):
            t = dot(rows_of(0), mall[0, :, n0:n1])
            for b in range(1, 4):
                t += dot(rows_of(b), mall[b, :, n0:n1])
            mine = rows_of(a)
            t += dot(mine, mall[4, :, n0:n1]) + dot(mine, mall[5, :, n0:n1])
            for k, h in enumerate(split3(t)):
                tt[k, :, n0:n1] = h
        t0, t1, t2 = tt[0], tt[1], tt[2]
        same = dot_nt(t0, t0) + dot_nt(t1, t1)
        cross = dot_nt(t0, t1) + dot_nt(t0, t2)
        if ii == 0:
            ks[...] = same
            kx[...] = cross
        else:
            cross = kx[...] + cross
            ks[...] += same + cross + jnp.transpose(cross)

    t_and_k(0)
    for j in range(3):
        remote(fsend, frecv.at[planes[j]], f_send.at[j], f_recv.at[planes[j]], (planes[j], o)).wait_recv()
    weights = times_metric(lanes_of([frecv[b] for b in range(4)]))
    w_row = as_row(2.0 * weights)

    lane = lax.broadcasted_iota(jnp.int32, (8, 128), 1)
    w0, w1 = jnp.broadcast_to(w_row[:, :128], (8, 128)), jnp.broadcast_to(w_row[:, 128:224], (8, 96))

    zero32 = jnp.zeros((8, 32), F32)

    def coul(k, carry):
        for j in range(4):
            rows = pl.ds(pl.multiple_of(k * 32 + 8 * j, 8), 8)
            acc = jnp.zeros((8, 128), F32)
            for m in range(80):
                z = jnp.concatenate([bb[m, rows, 128:224] * w1, zero32], axis=1)
                col = jnp.sum(bb[m, rows, 0:128] * w0 + z, axis=1, keepdims=True)
                acc = jnp.where(lane == m, col, acc)
            jacc[rows, :] = acc[:, :80]
        return carry

    lax.fori_loop(0, 10, coul, 0)
    jt = jnp.transpose(jacc[...])

    t_and_k(1)

    def packed(x):
        tail = jnp.concatenate([x[56:, :48], jnp.concatenate([x[56:, 48:], jnp.zeros((24, 16), F32)], axis=1),
                                jnp.zeros((8, 48), F32)], axis=0)
        return jnp.concatenate([x[:56], tail], axis=1)

    for c in range(4):
        for k in range(4):
            gs[k % 2, k // 2, c] = packed(jnp.where(o == k, jt[:, 80 * c:80 * c + 80], 0.0)
                                          - ks[80 * k:80 * k + 80, 80 * c:80 * c + 80])
    pair = remote(gs.at[1 - core], gp, p_sems.at[0], p_sems.at[1], (a, core_mate))
    pair.start()
    pair.wait()
    gf[...] = gs[core] + gp[...]

    def r_copy(k):
        plane, y = planes[k // 2], (row_y + k % 2) % 2
        return remote(gf.at[y, plane], gr.at[a, row_y], r_send.at[k], r_recv.at[a, row_y], (plane, 2 * y + core))

    r_order = (0, 1, 2, 3, 4, 5, 7)
    for k in r_order:
        r_copy(k).start()
    total = gf[row_y, a]
    for k in r_order:
        plane, y = planes[k // 2], (row_y + k % 2) % 2
        remote(gf.at[y, plane], gr.at[plane, y], r_send.at[k], r_recv.at[plane, y], (plane, 2 * y + core)).wait_recv()
        total = total + gr[plane, y]
    out_ref[0] = jnp.concatenate([total[:, :80], jnp.concatenate([total[0:24, 80:128], total[24:48, 80:112]], axis=1)], axis=0)


    for dest in peers:
        main_copy(dest, pl.ds(0, 80)).wait_send()
        rest_copy(0, dest).wait_send()
        rest_copy(1, dest).wait_send()
        g_copy(dest).wait_send()
    for k in r_order:
        r_copy(k).wait_send()
    for r in range(3):
        relay(r, 'drain')
    for j in range(3):
        f_copy(j).wait_send()
        for k in range(3):
            mf_copy(planes[j], o, o, k).wait_send()


def solution(mesh):
    def local_fock(ints_blk, metric_blk, orbitals):
        dma = pltpu.SemaphoreType.DMA
        return pl.pallas_call(
            kernel,
            name='fock',
            out_shape=jax.ShapeDtypeStruct((1, 80, 80), F32),
            in_specs=[pl.BlockSpec(memory_space=pl.ANY), pl.BlockSpec(memory_space=pl.ANY),
                      pl.BlockSpec(memory_space=pltpu.VMEM)],
            out_specs=pl.BlockSpec(memory_space=pltpu.VMEM),
            scratch_shapes=[
                pltpu.VMEM((80, 320, 224), F32),
                pltpu.VMEM((2, 512, 128), F32),
                pltpu.VMEM((32, 80, 128), BF16),
                pltpu.VMEM((32, 16, 512), BF16),
                pltpu.VMEM((2, 16, 80, 128), BF16),
                pltpu.VMEM((2, 16, 16, 512), BF16),
                pltpu.VMEM((16, 80, 128), BF16),
                pltpu.VMEM((6, 256, 896), BF16),
                pltpu.VMEM((224, 896), F32),
                pltpu.VMEM((80, 32, 128), F32),
                pltpu.VMEM((96, 1024), BF16),
                pltpu.VMEM((3, 320, 896), BF16),
                pltpu.VMEM((320, 320), F32),
                pltpu.VMEM((320, 320), F32),
                pltpu.VMEM((320, 80), F32),
                pltpu.VMEM((32, 256), F32),
                pltpu.VMEM((1, 256), F32),
                pltpu.VMEM((16, 1, 256), F32),
                pltpu.VMEM((1, 256), F32),
                pltpu.VMEM((4, 1, 256), F32),
                pltpu.VMEM((2, 2, 4, 56, 128), F32),
                pltpu.VMEM((2, 4, 56, 128), F32),
                pltpu.VMEM((2, 4, 56, 128), F32),
                pltpu.VMEM((4, 2, 56, 128), F32),
                dma((20,)), dma(()),
                dma((3, 16)), dma((3, 16)),
                dma((4, 2)), dma((4,)),
                dma((4, 3)), dma((4, 4)),
                dma((16,)), dma((16,)),
                dma((3,)), dma((4,)),
                dma((2,)), dma((8,)), dma((4, 2)),
            ],
            compiler_params=pltpu.CompilerParams(collective_id=0, has_side_effects=True, vmem_limit_bytes=67043328),
        )(jnp.transpose(ints_blk, (1, 2, 0)), metric_blk, jnp.transpose(orbitals[0]))

    return jax.shard_map(local_fock, mesh=mesh, in_specs=(P(('sys', 'aux'), 'orb', None), P(('sys', 'aux'), None), P('sys', None, None)), out_specs=P('sys', 'orb', 'aux'), check_vma=False)
```

```python
import functools

import jax
import jax.numpy as jnp
from jax import lax
from jax.experimental import pallas as pl
from jax.experimental.pallas import tpu as pltpu
from jax.sharding import PartitionSpec as P

F32, BF16 = jnp.float32, jnp.bfloat16
MESH = pl.DeviceIdType.MESH
NT = (((1,), (1,)), ((), ()))
AHEAD = 8


def split3(x):
    h0 = x.astype(BF16)
    r1 = x - h0.astype(F32)
    h1 = r1.astype(BF16)
    r2 = r1 - h1.astype(F32)
    return h0, h1, r2.astype(BF16)


def dot(a, b):
    return jnp.dot(a, b, preferred_element_type=F32)


def dot_nt(a, b):
    return lax.dot_general(a, b, NT, preferred_element_type=F32)


def kernel(b_hbm, m_hbm, c_ref, out_ref, bb, stage, smain, srest, rmain, rrest, rest, mall, mown, cb, c3, tt, ks, kx, jacc, gam, gsend, grecv,
           fsend, frecv, gs, gp, gf, gr, b_sem, m_sem, s_send, s_recv, mz_send, mz_recv, mf_send, mf_recv, g_send, g_recv,
           f_send, f_recv, p_sems, r_send, r_recv):
    a, o = lax.axis_index('aux'), lax.axis_index('orb')
    me = a * 4 + o
    core, row_y = o % 2, o // 2
    core_mate, y_mate = o + 1 - 2 * core, (o + 2) % 4
    planes = [(a + 2) % 4, 3 - a, a + 1 - 2 * (a % 2), a]
    peers = [(planes[k // 4], (o + k % 4) % 4) for k in range(16) if k != 12]

    def remote(src, dst, send, recv, dest):
        return pltpu.make_async_remote_copy(src_ref=src, dst_ref=dst, send_sem=send, recv_sem=recv,
                                            device_id={'aux': dest[0], 'orb': dest[1]}, device_id_type=MESH)

    def b_copy(g):
        rows = pl.ds(g * 4, 4)
        return pltpu.make_async_copy(b_hbm.at[rows], bb.at[rows], b_sem.at[g])

    m_copy = pltpu.make_async_copy(m_hbm, mown, m_sem)
    m_copy.start()
    for g in range(2):
        b_copy(g).start()

    barrier = pltpu.get_barrier_semaphore()
    for dest in peers:
        pl.semaphore_signal(barrier, inc=1, device_id={'aux': dest[0], 'orb': dest[1]}, device_id_type=MESH)

    m_copy.wait()
    for g in range(2, AHEAD):
        b_copy(g).start()
    m0, m1, m2 = split3(mown[...])
    pad = jnp.zeros((32, 896), BF16)
    mall[pl.ds(a, 1), 0:224, :] = m0[None]
    mall[pl.ds(a, 1), 224:256, :] = pad[None]
    mall[4, 0:224, :] = m1
    mall[4, 224:256, :] = pad
    mall[5, 0:224, :] = m2
    mall[5, 224:256, :] = pad

    pl.semaphore_wait(barrier, 15)

    quarter = pl.ds(pl.multiple_of(o * 64, 64), 64)

    def mz_copy(plane, step):
        part = mall.at[plane, quarter, :]
        return remote(part, part, mz_send.at[plane, (step + 1) // 2], mz_recv.at[plane], (a + step, o))

    def mf_copy(plane, part_of, dest, k):
        part = mall.at[plane, pl.ds(pl.multiple_of(part_of * 64, 64), 64), :]
        return remote(part, part, mf_send.at[plane, k], mf_recv.at[plane, part_of], (a, dest))

    def relay(r, action):
        for step in (1, -1):
            plane = a - step * r

            @pl.when((plane >= 0) & (plane <= 3))
            def _():
                if action == 'send' and r > 0:
                    mz_copy(plane, step).wait_recv()
                if r < 3:
                    @pl.when((a + step >= 0) & (a + step <= 3))
                    def _():
                        cp = mz_copy(plane, step)
                        cp.start() if action == 'send' else cp.wait_send()
                if action == 'send' and r > 0:
                    mf_copy(plane, o, core_mate, 0).start()
                    mf_copy(plane, o, y_mate, 1).start()

    def pass_on(r):
        for step in (1, -1):
            plane = a - step * r

            @pl.when((plane >= 0) & (plane <= 3))
            def _():
                mf_copy(plane, y_mate, y_mate, 2).wait_recv()
                mf_copy(plane, y_mate, core_mate, 2).start()

    relay(0, 'send')

    def main_copy(ii, dest, rows):
        d = dest[0] * 4 + dest[1]
        return remote(smain.at[2 * d + ii, rows, :], rmain.at[ii, me, rows, :], s_send.at[2 + ii, d], s_recv.at[2 + ii, me],
                      dest)

    def rest_copy(ii, dest):
        d = dest[0] * 4 + dest[1]
        return remote(srest.at[2 * d + ii], rrest.at[ii, me], s_send.at[ii, d], s_recv.at[ii, me], dest)

    parts = split3(c_ref[...])
    zero = jnp.zeros((32, 320), BF16)
    for k in range(3):
        rows = [parts[k] if j <= 2 - k else zero for j in range(3)]
        c3[32 * k:32 * k + 32, :] = jnp.concatenate(rows + [zero[:, :64]], axis=1)
    own = jnp.zeros((32, 80), F32)
    for k in range(4):
        own = jnp.where(o == k, c_ref[:, 80 * k:80 * k + 80], own)
    for m in range(80):
        cb[m] = jnp.broadcast_to(own[:, m:m + 1], (32, 128))
    rest[...] = jnp.zeros((16, 80, 128), BF16)
    srest[:, :, 384:512] = jnp.zeros((32, 16, 128), BF16)
    gam[...] = jnp.zeros((32, 256), F32)

    def group(g, carry):
        for k in range(2):
            b_copy(2 * g + k).wait()

        @pl.when(2 * g + AHEAD < 20)
        def _():
            for k in range(2):
                b_copy(2 * g + k + AHEAD).start()

        base = lax.rem(g, 2) * 8

        def rows4(k, carry):
            part0 = part1 = None
            for j in range(4):
                m = 4 * k + j
                w = jnp.concatenate(list(split3(bb[g * 8 + m])) + [jnp.zeros((64, 224), BF16)], axis=0)
                r = dot(c3[...], w)
                h = r[0:32] + r[32:64] + r[64:96]
                stage[0, pl.ds(base + m, 32, stride=16), :] = h[:, :128]
                stage[1, pl.ds(base + m, 32, stride=16), 0:96] = h[:, 128:]
                coef = cb[g * 8 + m]
                add0, add1 = h[:, :128] * coef, h[:, 128:] * coef[:, :96]
                part0 = add0 if part0 is None else part0 + add0
                part1 = add1 if part1 is None else part1 + add1
            gam[:, 0:128] += part0
            gam[:, 128:224] += part1
            return carry

        lax.fori_loop(0, 2, rows4, 0)

        @pl.when(lax.rem(g, 2) == 1)
        def _():
            rows = pl.ds(pl.multiple_of((g // 2) * 16, 16), 16)
            smain[:, rows, :] = stage[0].reshape(32, 16, 128).astype(BF16)
            for dest in peers:
                main_copy(0, dest, rows).start()

        for c in range(5):
            @pl.when(g == 2 * c + 1)
            def _():
                at = 96 * c if c < 4 else 384
                srest[:, :, at:at + 96] = stage[1].reshape(32, 16, 128)[:, :, :96].astype(BF16)

        @pl.when(g == 4)
        def _():
            relay(1, 'send')

        return carry

    lax.fori_loop(0, 10, group, 0)

    def g_copy(dest):
        return remote(gsend, grecv.at[me], g_send.at[dest[0] * 4 + dest[1]], g_recv.at[me], dest)

    g_row = jnp.sum(gam[...], axis=0, keepdims=True)
    gsend[...] = g_row
    grecv[pl.ds(me, 1)] = g_row[None]
    for dest in peers:
        g_copy(dest).start()

    for dest in peers:
        rest_copy(0, dest).start()
    relay(2, 'send')
    pass_on(1)
    for dest in peers:
        main_copy(1, dest, pl.ds(0, 32)).start()
    rmain[:, pl.ds(me, 1)] = smain[pl.ds(2 * me, 2)][:, None]
    rrest[:, pl.ds(me, 1)] = srest[pl.ds(2 * me, 2)][:, None]

    def lanes_of(rows):
        return jnp.concatenate([r[:, :224] for r in rows], axis=1)

    def as_row(col):
        x = jnp.broadcast_to(col, (224, 128))
        return jnp.concatenate([jnp.transpose(x[:128])[0:1], jnp.transpose(x[96:])[0:1, 32:], jnp.zeros((1, 32), F32)],
                               axis=1)

    def times_metric(row):
        return jnp.sum(mown[...] * row, axis=1, keepdims=True)

    for s in peers:
        remote(gsend, grecv.at[s[0] * 4 + s[1]], g_send.at[0], g_recv.at[s[0] * 4 + s[1]], s).wait_recv()
    gamma = lanes_of([grecv[4 * b] + grecv[4 * b + 1] + grecv[4 * b + 2] + grecv[4 * b + 3] for b in range(4)])
    fit_row = as_row(times_metric(gamma))
    fsend[...] = fit_row
    frecv[pl.ds(a, 1)] = fit_row[None]

    def f_copy(j):
        return remote(fsend, frecv.at[a], f_send.at[j], f_recv.at[a], (planes[j], o))

    for j in range(3):
        f_copy(j).start()
    for dest in peers:
        main_copy(1, dest, pl.ds(32, 48)).start()
        rest_copy(1, dest).start()
    relay(3, 'send')
    pass_on(2)
    pass_on(3)

    for r in range(1, 4):
        for step in (1, -1):
            plane = a - step * r

            @pl.when((plane >= 0) & (plane <= 3))
            def _():
                for part_of in (core_mate, 3 - o):
                    mf_copy(plane, part_of, part_of, 0).wait_recv()

    def t_and_k(ii):
        for s in peers:
            n = s[0] * 4 + s[1]
            remote(smain.at[ii], rmain.at[ii, n], s_send.at[2 + ii, n], s_recv.at[2 + ii, n], s).wait_recv()
            remote(srest.at[ii], rrest.at[ii, n], s_send.at[ii, n], s_recv.at[ii, n], s).wait_recv()
        for n in range(16):
            for c in range(5):
                at = 96 * c if c < 4 else 384
                rest[n, 16 * c:16 * c + 16, 0:96] = rrest[ii, n, :, at:at + 96]

        def rows_of(plane):
            four = pl.ds(4 * plane, 4)
            return jnp.concatenate([rmain[ii, four].reshape(320, 128), rest[four].reshape(320, 128)], axis=1)

        for n0, n1 in ((0, 256), (256, 512), (512, 768), (768, 896)):
            t = dot(rows_of(0), mall[0, :, n0:n1])
            for b in range(1, 4):
                t += dot(rows_of(b), mall[b, :, n0:n1])
            mine = rows_of(a)
            t += dot(mine, mall[4, :, n0:n1]) + dot(mine, mall[5, :, n0:n1])
            for k, h in enumerate(split3(t)):
                tt[k, :, n0:n1] = h
        t0, t1, t2 = tt[0], tt[1], tt[2]
        same = dot_nt(t0, t0) + dot_nt(t1, t1)
        cross = dot_nt(t0, t1) + dot_nt(t0, t2)
        if ii == 0:
            ks[...] = same
            kx[...] = cross
        else:
            cross = kx[...] + cross
            ks[...] += same + cross + jnp.transpose(cross)

    t_and_k(0)
    for j in range(3):
        remote(fsend, frecv.at[planes[j]], f_send.at[j], f_recv.at[planes[j]], (planes[j], o)).wait_recv()
    weights = times_metric(lanes_of([frecv[b] for b in range(4)]))
    w_row = as_row(2.0 * weights)

    lane = lax.broadcasted_iota(jnp.int32, (8, 128), 1)
    w0, w1 = jnp.broadcast_to(w_row[:, :128], (8, 128)), jnp.broadcast_to(w_row[:, 128:224], (8, 96))

    zero32 = jnp.zeros((8, 32), F32)

    def coul(k, carry):
        for j in range(4):
            rows = pl.ds(pl.multiple_of(k * 32 + 8 * j, 8), 8)
            acc = jnp.zeros((8, 128), F32)
            for m in range(80):
                z = jnp.concatenate([bb[m, rows, 128:224] * w1, zero32], axis=1)
                col = jnp.sum(bb[m, rows, 0:128] * w0 + z, axis=1, keepdims=True)
                acc = jnp.where(lane == m, col, acc)
            jacc[rows, :] = acc[:, :80]
        return carry

    lax.fori_loop(0, 10, coul, 0)
    jt = jnp.transpose(jacc[...])

    t_and_k(1)

    def packed(x):
        tail = jnp.concatenate([x[56:, :48], jnp.concatenate([x[56:, 48:], jnp.zeros((24, 16), F32)], axis=1),
                                jnp.zeros((8, 48), F32)], axis=0)
        return jnp.concatenate([x[:56], tail], axis=1)

    for c in range(4):
        for k in range(4):
            gs[k % 2, k // 2, c] = packed(jnp.where(o == k, jt[:, 80 * c:80 * c + 80], 0.0)
                                          - ks[80 * k:80 * k + 80, 80 * c:80 * c + 80])
    pair = remote(gs.at[1 - core], gp, p_sems.at[0], p_sems.at[1], (a, core_mate))
    pair.start()
    pair.wait()
    gf[...] = gs[core] + gp[...]

    def r_copy(k):
        plane, y = planes[k // 2], (row_y + k % 2) % 2
        return remote(gf.at[y, plane], gr.at[a, row_y], r_send.at[k], r_recv.at[a, row_y], (plane, 2 * y + core))

    r_order = (0, 1, 2, 3, 4, 5, 7)
    for k in r_order:
        r_copy(k).start()
    total = gf[row_y, a]
    for k in r_order:
        plane, y = planes[k // 2], (row_y + k % 2) % 2
        remote(gf.at[y, plane], gr.at[plane, y], r_send.at[k], r_recv.at[plane, y], (plane, 2 * y + core)).wait_recv()
        total = total + gr[plane, y]
    out_ref[0] = jnp.concatenate([total[:, :80], jnp.concatenate([total[0:24, 80:128], total[24:48, 80:112]], axis=1)], axis=0)


    for dest in peers:
        main_copy(0, dest, pl.ds(0, 80)).wait_send()
        main_copy(1, dest, pl.ds(0, 80)).wait_send()
        rest_copy(0, dest).wait_send()
        rest_copy(1, dest).wait_send()
        g_copy(dest).wait_send()
    for k in r_order:
        r_copy(k).wait_send()
    for r in range(3):
        relay(r, 'drain')
    for j in range(3):
        f_copy(j).wait_send()
        for k in range(3):
            mf_copy(planes[j], o, o, k).wait_send()


def solution(mesh):
    def local_fock(ints_blk, metric_blk, orbitals):
        dma = pltpu.SemaphoreType.DMA
        return pl.pallas_call(
            kernel,
            name='fock',
            out_shape=jax.ShapeDtypeStruct((1, 80, 80), F32),
            in_specs=[pl.BlockSpec(memory_space=pl.ANY), pl.BlockSpec(memory_space=pl.ANY),
                      pl.BlockSpec(memory_space=pltpu.VMEM)],
            out_specs=pl.BlockSpec(memory_space=pltpu.VMEM),
            scratch_shapes=[
                pltpu.VMEM((80, 320, 224), F32),
                pltpu.VMEM((2, 512, 128), F32),
                pltpu.VMEM((32, 80, 128), BF16),
                pltpu.VMEM((32, 16, 512), BF16),
                pltpu.VMEM((2, 16, 80, 128), BF16),
                pltpu.VMEM((2, 16, 16, 512), BF16),
                pltpu.VMEM((16, 80, 128), BF16),
                pltpu.VMEM((6, 256, 896), BF16),
                pltpu.VMEM((224, 896), F32),
                pltpu.VMEM((80, 32, 128), F32),
                pltpu.VMEM((96, 1024), BF16),
                pltpu.VMEM((3, 320, 896), BF16),
                pltpu.VMEM((320, 320), F32),
                pltpu.VMEM((320, 320), F32),
                pltpu.VMEM((320, 80), F32),
                pltpu.VMEM((32, 256), F32),
                pltpu.VMEM((1, 256), F32),
                pltpu.VMEM((16, 1, 256), F32),
                pltpu.VMEM((1, 256), F32),
                pltpu.VMEM((4, 1, 256), F32),
                pltpu.VMEM((2, 2, 4, 56, 128), F32),
                pltpu.VMEM((2, 4, 56, 128), F32),
                pltpu.VMEM((2, 4, 56, 128), F32),
                pltpu.VMEM((4, 2, 56, 128), F32),
                dma((20,)), dma(()),
                dma((4, 16)), dma((4, 16)),
                dma((4, 2)), dma((4,)),
                dma((4, 3)), dma((4, 4)),
                dma((16,)), dma((16,)),
                dma((3,)), dma((4,)),
                dma((2,)), dma((8,)), dma((4, 2)),
            ],
            compiler_params=pltpu.CompilerParams(collective_id=0, has_side_effects=True, vmem_limit_bytes=67043328),
        )(jnp.transpose(ints_blk, (1, 2, 0)), metric_blk, jnp.transpose(orbitals[0]))

    return jax.shard_map(local_fock, mesh=mesh, in_specs=(P(('sys', 'aux'), 'orb', None), P(('sys', 'aux'), None), P('sys', None, None)), out_specs=P('sys', 'orb', 'aux'), check_vma=False)
```

```python
import functools

import jax
import jax.numpy as jnp
from jax import lax
from jax.experimental import pallas as pl
from jax.experimental.pallas import tpu as pltpu
from jax.sharding import PartitionSpec as P

F32, BF16 = jnp.float32, jnp.bfloat16
MESH = pl.DeviceIdType.MESH
NT = (((1,), (1,)), ((), ()))
AHEAD = 8


def split3(x):
    h0 = x.astype(BF16)
    r1 = x - h0.astype(F32)
    h1 = r1.astype(BF16)
    r2 = r1 - h1.astype(F32)
    return h0, h1, r2.astype(BF16)


def dot(a, b):
    return jnp.dot(a, b, preferred_element_type=F32)


def dot_nt(a, b):
    return lax.dot_general(a, b, NT, preferred_element_type=F32)


def kernel(b_hbm, m_hbm, c_ref, out_ref, bb, stage, smain, srest, rmain, rrest, rest, mall, mown, cb, c3, tt, ks, kx, jacc, gam, gsend, grecv,
           fsend, frecv, gs, gp, gf, gr, b_sem, m_sem, s_send, s_recv, mz_send, mz_recv, mf_send, mf_recv, g_send, g_recv,
           f_send, f_recv, p_sems, r_send, r_recv):
    a, o = lax.axis_index('aux'), lax.axis_index('orb')
    me = a * 4 + o
    core, row_y = o % 2, o // 2
    core_mate, y_mate = o + 1 - 2 * core, (o + 2) % 4
    planes = [(a + 2) % 4, 3 - a, a + 1 - 2 * (a % 2), a]
    peers = [(planes[k // 4], (o + k % 4) % 4) for k in range(16) if k != 12]

    def remote(src, dst, send, recv, dest):
        return pltpu.make_async_remote_copy(src_ref=src, dst_ref=dst, send_sem=send, recv_sem=recv,
                                            device_id={'aux': dest[0], 'orb': dest[1]}, device_id_type=MESH)

    def b_copy(g):
        rows = pl.ds(g * 4, 4)
        return pltpu.make_async_copy(b_hbm.at[rows], bb.at[rows], b_sem.at[g])

    m_copy = pltpu.make_async_copy(m_hbm, mown, m_sem)
    m_copy.start()
    for g in range(2):
        b_copy(g).start()

    barrier = pltpu.get_barrier_semaphore()
    for dest in peers:
        pl.semaphore_signal(barrier, inc=1, device_id={'aux': dest[0], 'orb': dest[1]}, device_id_type=MESH)

    m_copy.wait()
    for g in range(2, AHEAD):
        b_copy(g).start()
    m0, m1, m2 = split3(mown[...])
    pad = jnp.zeros((32, 896), BF16)
    mall[pl.ds(a, 1), 0:224, :] = m0[None]
    mall[pl.ds(a, 1), 224:256, :] = pad[None]
    mall[4, 0:224, :] = m1
    mall[4, 224:256, :] = pad
    mall[5, 0:224, :] = m2
    mall[5, 224:256, :] = pad

    pl.semaphore_wait(barrier, 15)

    quarter = pl.ds(pl.multiple_of(o * 64, 64), 64)

    def mz_copy(plane, step):
        part = mall.at[plane, quarter, :]
        return remote(part, part, mz_send.at[plane, (step + 1) // 2], mz_recv.at[plane], (a + step, o))

    def mf_copy(plane, part_of, dest, k):
        part = mall.at[plane, pl.ds(pl.multiple_of(part_of * 64, 64), 64), :]
        return remote(part, part, mf_send.at[plane, k], mf_recv.at[plane, part_of], (a, dest))

    def relay(r, action):
        for step in (1, -1):
            plane = a - step * r

            @pl.when((plane >= 0) & (plane <= 3))
            def _():
                if action == 'send' and r > 0:
                    mz_copy(plane, step).wait_recv()
                if r < 3:
                    @pl.when((a + step >= 0) & (a + step <= 3))
                    def _():
                        cp = mz_copy(plane, step)
                        cp.start() if action == 'send' else cp.wait_send()
                if action == 'send' and r > 0:
                    mf_copy(plane, o, core_mate, 0).start()
                    mf_copy(plane, o, y_mate, 1).start()

    def pass_on(r):
        for step in (1, -1):
            plane = a - step * r

            @pl.when((plane >= 0) & (plane <= 3))
            def _():
                mf_copy(plane, y_mate, y_mate, 2).wait_recv()
                mf_copy(plane, y_mate, core_mate, 2).start()

    relay(0, 'send')

    def main_copy(ii, dest, rows):
        d = dest[0] * 4 + dest[1]
        return remote(smain.at[2 * d + ii, rows, :], rmain.at[ii, me, rows, :], s_send.at[2 + ii, d], s_recv.at[2 + ii, me],
                      dest)

    def rest_copy(ii, dest):
        d = dest[0] * 4 + dest[1]
        return remote(srest.at[2 * d + ii], rrest.at[ii, me], s_send.at[ii, d], s_recv.at[ii, me], dest)

    parts = split3(c_ref[...])
    zero = jnp.zeros((32, 320), BF16)
    for k in range(3):
        rows = [parts[k] if j <= 2 - k else zero for j in range(3)]
        c3[32 * k:32 * k + 32, :] = jnp.concatenate(rows + [zero[:, :64]], axis=1)
    own = jnp.zeros((32, 80), F32)
    for k in range(4):
        own = jnp.where(o == k, c_ref[:, 80 * k:80 * k + 80], own)
    for m in range(80):
        cb[m] = jnp.broadcast_to(own[:, m:m + 1], (32, 128))
    rest[...] = jnp.zeros((16, 80, 128), BF16)
    srest[:, :, 384:512] = jnp.zeros((32, 16, 128), BF16)
    gam[...] = jnp.zeros((32, 256), F32)

    def group(g, carry):
        for k in range(2):
            b_copy(2 * g + k).wait()

        @pl.when(2 * g + AHEAD < 20)
        def _():
            for k in range(2):
                b_copy(2 * g + k + AHEAD).start()

        base = lax.rem(g, 2) * 8

        def rows4(k, carry):
            part0 = part1 = None
            for j in range(4):
                m = 4 * k + j
                w = jnp.concatenate(list(split3(bb[g * 8 + m])) + [jnp.zeros((64, 224), BF16)], axis=0)
                r = dot(c3[...], w)
                h = r[0:32] + r[32:64] + r[64:96]
                stage[0, pl.ds(base + m, 32, stride=16), :] = h[:, :128]
                stage[1, pl.ds(base + m, 32, stride=16), 0:96] = h[:, 128:]
                coef = cb[g * 8 + m]
                add0, add1 = h[:, :128] * coef, h[:, 128:] * coef[:, :96]
                part0 = add0 if part0 is None else part0 + add0
                part1 = add1 if part1 is None else part1 + add1
            gam[:, 0:128] += part0
            gam[:, 128:224] += part1
            return carry

        lax.fori_loop(0, 2, rows4, 0)

        @pl.when(lax.rem(g, 2) == 1)
        def _():
            rows = pl.ds(pl.multiple_of((g // 2) * 16, 16), 16)
            smain[:, rows, :] = stage[0].reshape(32, 16, 128).astype(BF16)
            for dest in peers:
                main_copy(0, dest, rows).start()

        for c in range(5):
            @pl.when(g == 2 * c + 1)
            def _():
                at = 96 * c if c < 4 else 384
                srest[:, :, at:at + 96] = stage[1].reshape(32, 16, 128)[:, :, :96].astype(BF16)

        @pl.when(g == 4)
        def _():
            relay(1, 'send')

        return carry

    lax.fori_loop(0, 10, group, 0)

    def g_copy(dest):
        return remote(gsend, grecv.at[me], g_send.at[dest[0] * 4 + dest[1]], g_recv.at[me], dest)

    g_row = jnp.sum(gam[...], axis=0, keepdims=True)
    gsend[...] = g_row
    grecv[pl.ds(me, 1)] = g_row[None]
    for dest in peers:
        g_copy(dest).start()

    for dest in peers:
        rest_copy(0, dest).start()
    relay(2, 'send')
    pass_on(1)
    for dest in peers:
        main_copy(1, dest, pl.ds(0, 32)).start()
    rmain[:, pl.ds(me, 1)] = smain[pl.ds(2 * me, 2)][:, None]
    rrest[:, pl.ds(me, 1)] = srest[pl.ds(2 * me, 2)][:, None]

    def lanes_of(rows):
        return jnp.concatenate([r[:, :224] for r in rows], axis=1)

    def as_row(col):
        x = jnp.broadcast_to(col, (224, 128))
        return jnp.concatenate([jnp.transpose(x[:128])[0:1], jnp.transpose(x[96:])[0:1, 32:], jnp.zeros((1, 32), F32)],
                               axis=1)

    def times_metric(row):
        return jnp.sum(mown[...] * row, axis=1, keepdims=True)

    for s in peers:
        remote(gsend, grecv.at[s[0] * 4 + s[1]], g_send.at[0], g_recv.at[s[0] * 4 + s[1]], s).wait_recv()
    gamma = lanes_of([grecv[4 * b] + grecv[4 * b + 1] + grecv[4 * b + 2] + grecv[4 * b + 3] for b in range(4)])
    fit_row = as_row(times_metric(gamma))
    fsend[...] = fit_row
    frecv[pl.ds(a, 1)] = fit_row[None]

    def f_copy(j):
        return remote(fsend, frecv.at[a], f_send.at[j], f_recv.at[a], (planes[j], o))

    for j in range(3):
        f_copy(j).start()
    for dest in peers:
        main_copy(1, dest, pl.ds(32, 48)).start()
        rest_copy(1, dest).start()
    relay(3, 'send')
    pass_on(2)
    pass_on(3)

    for r in range(1, 4):
        for step in (1, -1):
            plane = a - step * r

            @pl.when((plane >= 0) & (plane <= 3))
            def _():
                for part_of in (core_mate, 3 - o):
                    mf_copy(plane, part_of, part_of, 0).wait_recv()

    def t_and_k(ii):
        for s in peers:
            n = s[0] * 4 + s[1]
            remote(smain.at[ii], rmain.at[ii, n], s_send.at[2 + ii, n], s_recv.at[2 + ii, n], s).wait_recv()
            remote(srest.at[ii], rrest.at[ii, n], s_send.at[ii, n], s_recv.at[ii, n], s).wait_recv()
        for n in range(16):
            for c in range(5):
                at = 96 * c if c < 4 else 384
                rest[n, 16 * c:16 * c + 16, 0:96] = rrest[ii, n, :, at:at + 96]

        def rows_of(plane):
            four = pl.ds(4 * plane, 4)
            return jnp.concatenate([rmain[ii, four].reshape(320, 128), rest[four].reshape(320, 128)], axis=1)

        for n0, n1 in ((0, 256), (256, 512), (512, 768), (768, 896)):
            t = dot(rows_of(0), mall[0, :, n0:n1])
            for b in range(1, 4):
                t += dot(rows_of(b), mall[b, :, n0:n1])
            mine = rows_of(a)
            t += dot(mine, mall[4, :, n0:n1]) + dot(mine, mall[5, :, n0:n1])
            for k, h in enumerate(split3(t)):
                tt[k, :, n0:n1] = h
        t0, t1, t2 = tt[0], tt[1], tt[2]
        same = dot_nt(t0, t0) + dot_nt(t1, t1)
        cross = dot_nt(t0, t1) + dot_nt(t0, t2)
        if ii == 0:
            ks[...] = same
            kx[...] = cross
        else:
            cross = kx[...] + cross
            ks[...] += same + cross + jnp.transpose(cross)

    t_and_k(0)
    for j in range(3):
        remote(fsend, frecv.at[planes[j]], f_send.at[j], f_recv.at[planes[j]], (planes[j], o)).wait_recv()
    weights = times_metric(lanes_of([frecv[b] for b in range(4)]))
    w_row = as_row(2.0 * weights)

    lane = lax.broadcasted_iota(jnp.int32, (8, 128), 1)
    w0, w1 = jnp.broadcast_to(w_row[:, :128], (8, 128)), jnp.broadcast_to(w_row[:, 128:224], (8, 96))

    zero32 = jnp.zeros((8, 32), F32)

    def coul(k, carry):
        for j in range(4):
            rows = pl.ds(pl.multiple_of(k * 32 + 8 * j, 8), 8)
            acc = jnp.zeros((8, 128), F32)
            for m in range(80):
                z = jnp.concatenate([bb[m, rows, 128:224] * w1, zero32], axis=1)
                col = jnp.sum(bb[m, rows, 0:128] * w0 + z, axis=1, keepdims=True)
                acc = jnp.where(lane == m, col, acc)
            jacc[rows, :] = acc[:, :80]
        return carry

    lax.fori_loop(0, 10, coul, 0)
    jt = jnp.transpose(jacc[...])

    t_and_k(1)

    def packed(x):
        tail = jnp.concatenate([x[56:, :48], jnp.concatenate([x[56:, 48:], jnp.zeros((24, 16), F32)], axis=1),
                                jnp.zeros((8, 48), F32)], axis=0)
        return jnp.concatenate([x[:56], tail], axis=1)

    for c in range(4):
        for k in range(4):
            gs[k % 2, k // 2, c] = packed(jnp.where(o == k, jt[:, 80 * c:80 * c + 80], 0.0)
                                          - ks[80 * k:80 * k + 80, 80 * c:80 * c + 80])
    far = 2 * (1 - a // 2)
    halves = [pl.ds(far, 2), pl.ds(2 - far, 2)]
    pairs = [remote(gs.at[1 - core, :, half], gp.at[:, half], p_sems.at[0, k], p_sems.at[1, k], (a, core_mate))
             for k, half in enumerate(halves)]
    for cp in pairs:
        cp.start()

    def r_copy(k):
        plane, y = planes[k // 2], (row_y + k % 2) % 2
        return remote(gf.at[y, plane], gr.at[a, row_y], r_send.at[k], r_recv.at[a, row_y], (plane, 2 * y + core))

    r_order = (0, 1, 2, 3, 4, 5, 7)
    for j, half in enumerate(halves):
        pairs[j].wait()
        gf[:, half] = gs[core, :, half] + gp[:, half]
        for k in r_order[4 * j:4 * j + 4]:
            r_copy(k).start()
    total = gf[row_y, a]
    for k in r_order:
        plane, y = planes[k // 2], (row_y + k % 2) % 2
        remote(gf.at[y, plane], gr.at[plane, y], r_send.at[k], r_recv.at[plane, y], (plane, 2 * y + core)).wait_recv()
        total = total + gr[plane, y]
    out_ref[0] = jnp.concatenate([total[:, :80], jnp.concatenate([total[0:24, 80:128], total[24:48, 80:112]], axis=1)], axis=0)


    for dest in peers:
        main_copy(0, dest, pl.ds(0, 80)).wait_send()
        main_copy(1, dest, pl.ds(0, 80)).wait_send()
        rest_copy(0, dest).wait_send()
        rest_copy(1, dest).wait_send()
        g_copy(dest).wait_send()
    for k in r_order:
        r_copy(k).wait_send()
    for r in range(3):
        relay(r, 'drain')
    for j in range(3):
        f_copy(j).wait_send()
        for k in range(3):
            mf_copy(planes[j], o, o, k).wait_send()


def solution(mesh):
    def local_fock(ints_blk, metric_blk, orbitals):
        dma = pltpu.SemaphoreType.DMA
        return pl.pallas_call(
            kernel,
            name='fock',
            out_shape=jax.ShapeDtypeStruct((1, 80, 80), F32),
            in_specs=[pl.BlockSpec(memory_space=pl.ANY), pl.BlockSpec(memory_space=pl.ANY),
                      pl.BlockSpec(memory_space=pltpu.VMEM)],
            out_specs=pl.BlockSpec(memory_space=pltpu.VMEM),
            scratch_shapes=[
                pltpu.VMEM((80, 320, 224), F32),
                pltpu.VMEM((2, 512, 128), F32),
                pltpu.VMEM((32, 80, 128), BF16),
                pltpu.VMEM((32, 16, 512), BF16),
                pltpu.VMEM((2, 16, 80, 128), BF16),
                pltpu.VMEM((2, 16, 16, 512), BF16),
                pltpu.VMEM((16, 80, 128), BF16),
                pltpu.VMEM((6, 256, 896), BF16),
                pltpu.VMEM((224, 896), F32),
                pltpu.VMEM((80, 32, 128), F32),
                pltpu.VMEM((96, 1024), BF16),
                pltpu.VMEM((3, 320, 896), BF16),
                pltpu.VMEM((320, 320), F32),
                pltpu.VMEM((320, 320), F32),
                pltpu.VMEM((320, 80), F32),
                pltpu.VMEM((32, 256), F32),
                pltpu.VMEM((1, 256), F32),
                pltpu.VMEM((16, 1, 256), F32),
                pltpu.VMEM((1, 256), F32),
                pltpu.VMEM((4, 1, 256), F32),
                pltpu.VMEM((2, 2, 4, 56, 128), F32),
                pltpu.VMEM((2, 4, 56, 128), F32),
                pltpu.VMEM((2, 4, 56, 128), F32),
                pltpu.VMEM((4, 2, 56, 128), F32),
                dma((20,)), dma(()),
                dma((4, 16)), dma((4, 16)),
                dma((4, 2)), dma((4,)),
                dma((4, 3)), dma((4, 4)),
                dma((16,)), dma((16,)),
                dma((3,)), dma((4,)),
                dma((2, 2)), dma((8,)), dma((4, 2)),
            ],
            compiler_params=pltpu.CompilerParams(collective_id=0, has_side_effects=True, vmem_limit_bytes=67043328),
        )(jnp.transpose(ints_blk, (1, 2, 0)), metric_blk, jnp.transpose(orbitals[0]))

    return jax.shard_map(local_fock, mesh=mesh, in_specs=(P(('sys', 'aux'), 'orb', None), P(('sys', 'aux'), None), P('sys', None, None)), out_specs=P('sys', 'orb', 'aux'), check_vma=False)
```

```python
import functools

import jax
import jax.numpy as jnp
from jax import lax
from jax.experimental import pallas as pl
from jax.experimental.pallas import tpu as pltpu
from jax.sharding import PartitionSpec as P

F32, BF16 = jnp.float32, jnp.bfloat16
MESH = pl.DeviceIdType.MESH
NT = (((1,), (1,)), ((), ()))
AHEAD = 8


def split3(x):
    h0 = x.astype(BF16)
    r1 = x - h0.astype(F32)
    h1 = r1.astype(BF16)
    r2 = r1 - h1.astype(F32)
    return h0, h1, r2.astype(BF16)


def dot(a, b):
    return jnp.dot(a, b, preferred_element_type=F32)


def dot_nt(a, b):
    return lax.dot_general(a, b, NT, preferred_element_type=F32)


def kernel(b_hbm, m_hbm, c_ref, out_ref, bb, stage, smain, srest, rmain, rrest, rest, mall, mown, cb, c3, tt, ks, kx, jacc, gam, gsend, grecv,
           fsend, frecv, gs, gp, gf, gr, b_sem, m_sem, s_send, s_recv, mz_send, mz_recv, mf_send, mf_recv, g_send, g_recv,
           f_send, f_recv, p_sems, r_send, r_recv):
    a, o = lax.axis_index('aux'), lax.axis_index('orb')
    me = a * 4 + o
    core, row_y = o % 2, o // 2
    core_mate, y_mate = o + 1 - 2 * core, (o + 2) % 4
    planes = [(a + 2) % 4, 3 - a, a + 1 - 2 * (a % 2), a]
    peers = [(planes[k // 4], (o + k % 4) % 4) for k in range(16) if k != 12]

    def remote(src, dst, send, recv, dest):
        return pltpu.make_async_remote_copy(src_ref=src, dst_ref=dst, send_sem=send, recv_sem=recv,
                                            device_id={'aux': dest[0], 'orb': dest[1]}, device_id_type=MESH)

    def b_copy(g):
        rows = pl.ds(g * 4, 4)
        return pltpu.make_async_copy(b_hbm.at[rows], bb.at[rows], b_sem.at[g])

    m_copy = pltpu.make_async_copy(m_hbm, mown, m_sem)
    m_copy.start()
    for g in range(2):
        b_copy(g).start()

    barrier = pltpu.get_barrier_semaphore()
    for dest in peers:
        pl.semaphore_signal(barrier, inc=1, device_id={'aux': dest[0], 'orb': dest[1]}, device_id_type=MESH)

    m_copy.wait()
    for g in range(2, AHEAD):
        b_copy(g).start()
    m0, m1, m2 = split3(mown[...])
    pad = jnp.zeros((32, 896), BF16)
    mall[pl.ds(a, 1), 0:224, :] = m0[None]
    mall[pl.ds(a, 1), 224:256, :] = pad[None]
    mall[4, 0:224, :] = m1
    mall[4, 224:256, :] = pad
    mall[5, 0:224, :] = m2
    mall[5, 224:256, :] = pad

    pl.semaphore_wait(barrier, 15)

    quarter = pl.ds(pl.multiple_of(o * 64, 64), 64)

    def mz_copy(plane, step):
        part = mall.at[plane, quarter, :]
        return remote(part, part, mz_send.at[plane, (step + 1) // 2], mz_recv.at[plane], (a + step, o))

    def mf_copy(plane, part_of, dest, k):
        part = mall.at[plane, pl.ds(pl.multiple_of(part_of * 64, 64), 64), :]
        return remote(part, part, mf_send.at[plane, k], mf_recv.at[plane, part_of], (a, dest))

    def relay(r, action):
        for step in (1, -1):
            plane = a - step * r

            @pl.when((plane >= 0) & (plane <= 3))
            def _():
                if action == 'send' and r > 0:
                    mz_copy(plane, step).wait_recv()
                if r < 3:
                    @pl.when((a + step >= 0) & (a + step <= 3))
                    def _():
                        cp = mz_copy(plane, step)
                        cp.start() if action == 'send' else cp.wait_send()
                if action == 'send' and r > 0:
                    mf_copy(plane, o, core_mate, 0).start()
                    mf_copy(plane, o, y_mate, 1).start()

    def pass_on(r):
        for step in (1, -1):
            plane = a - step * r

            @pl.when((plane >= 0) & (plane <= 3))
            def _():
                mf_copy(plane, y_mate, y_mate, 2).wait_recv()
                mf_copy(plane, y_mate, core_mate, 2).start()

    relay(0, 'send')

    def main_copy(ii, dest, rows):
        d = dest[0] * 4 + dest[1]
        return remote(smain.at[2 * d + ii, rows, :], rmain.at[ii, me, rows, :], s_send.at[2 + ii, d], s_recv.at[2 + ii, me],
                      dest)

    def rest_copy(ii, dest):
        d = dest[0] * 4 + dest[1]
        return remote(srest.at[2 * d + ii], rrest.at[ii, me], s_send.at[ii, d], s_recv.at[ii, me], dest)

    parts = split3(c_ref[...])
    zero = jnp.zeros((32, 320), BF16)
    for k in range(3):
        rows = [parts[k] if j <= 2 - k else zero for j in range(3)]
        c3[32 * k:32 * k + 32, :] = jnp.concatenate(rows + [zero[:, :64]], axis=1)
    own = jnp.zeros((32, 80), F32)
    for k in range(4):
        own = jnp.where(o == k, c_ref[:, 80 * k:80 * k + 80], own)
    for m in range(80):
        cb[m] = jnp.broadcast_to(own[:, m:m + 1], (32, 128))
    rest[...] = jnp.zeros((16, 80, 128), BF16)
    srest[:, :, 384:512] = jnp.zeros((32, 16, 128), BF16)
    gam[...] = jnp.zeros((32, 256), F32)

    def group(g, carry):
        for k in range(2):
            b_copy(2 * g + k).wait()

        @pl.when(2 * g + AHEAD < 20)
        def _():
            for k in range(2):
                b_copy(2 * g + k + AHEAD).start()

        base = lax.rem(g, 2) * 8

        def rows4(k, carry):
            part0 = part1 = None
            for j in range(4):
                m = 4 * k + j
                w = jnp.concatenate(list(split3(bb[g * 8 + m])) + [jnp.zeros((64, 224), BF16)], axis=0)
                r = dot(c3[...], w)
                h = r[0:32] + r[32:64] + r[64:96]
                stage[0, pl.ds(base + m, 32, stride=16), :] = h[:, :128]
                stage[1, pl.ds(base + m, 32, stride=16), 0:96] = h[:, 128:]
                coef = cb[g * 8 + m]
                add0, add1 = h[:, :128] * coef, h[:, 128:] * coef[:, :96]
                part0 = add0 if part0 is None else part0 + add0
                part1 = add1 if part1 is None else part1 + add1
            gam[:, 0:128] += part0
            gam[:, 128:224] += part1
            return carry

        lax.fori_loop(0, 2, rows4, 0)

        @pl.when(lax.rem(g, 2) == 1)
        def _():
            rows = pl.ds(pl.multiple_of((g // 2) * 16, 16), 16)
            smain[:, rows, :] = stage[0].reshape(32, 16, 128).astype(BF16)
            for dest in peers:
                main_copy(0, dest, rows).start()

        for c in range(5):
            @pl.when(g == 2 * c + 1)
            def _():
                at = 96 * c if c < 4 else 384
                srest[:, :, at:at + 96] = stage[1].reshape(32, 16, 128)[:, :, :96].astype(BF16)

        @pl.when(g == 4)
        def _():
            relay(1, 'send')

        return carry

    lax.fori_loop(0, 10, group, 0)

    def g_copy(dest):
        return remote(gsend, grecv.at[me], g_send.at[dest[0] * 4 + dest[1]], g_recv.at[me], dest)

    g_row = jnp.sum(gam[...], axis=0, keepdims=True)
    gsend[...] = g_row
    grecv[pl.ds(me, 1)] = g_row[None]
    for dest in peers:
        g_copy(dest).start()

    for dest in peers:
        rest_copy(0, dest).start()
    relay(2, 'send')
    pass_on(1)
    rmain[:, pl.ds(me, 1)] = smain[pl.ds(2 * me, 2)][:, None]
    rrest[:, pl.ds(me, 1)] = srest[pl.ds(2 * me, 2)][:, None]

    def lanes_of(rows):
        return jnp.concatenate([r[:, :224] for r in rows], axis=1)

    def as_row(col):
        x = jnp.broadcast_to(col, (224, 128))
        return jnp.concatenate([jnp.transpose(x[:128])[0:1], jnp.transpose(x[96:])[0:1, 32:], jnp.zeros((1, 32), F32)],
                               axis=1)

    def times_metric(row):
        return jnp.sum(mown[...] * row, axis=1, keepdims=True)

    for s in peers:
        remote(gsend, grecv.at[s[0] * 4 + s[1]], g_send.at[0], g_recv.at[s[0] * 4 + s[1]], s).wait_recv()
    gamma = lanes_of([grecv[4 * b] + grecv[4 * b + 1] + grecv[4 * b + 2] + grecv[4 * b + 3] for b in range(4)])
    fit_row = as_row(times_metric(gamma))
    fsend[...] = fit_row
    frecv[pl.ds(a, 1)] = fit_row[None]

    def f_copy(j):
        return remote(fsend, frecv.at[a], f_send.at[j], f_recv.at[a], (planes[j], o))

    for j in range(3):
        f_copy(j).start()
    for dest in peers:
        main_copy(1, dest, pl.ds(0, 80)).start()
        rest_copy(1, dest).start()
    relay(3, 'send')
    pass_on(2)
    pass_on(3)

    for r in range(1, 4):
        for step in (1, -1):
            plane = a - step * r

            @pl.when((plane >= 0) & (plane <= 3))
            def _():
                for part_of in (core_mate, 3 - o):
                    mf_copy(plane, part_of, part_of, 0).wait_recv()

    def t_and_k(ii):
        for s in peers:
            n = s[0] * 4 + s[1]
            remote(smain.at[ii], rmain.at[ii, n], s_send.at[2 + ii, n], s_recv.at[2 + ii, n], s).wait_recv()
            remote(srest.at[ii], rrest.at[ii, n], s_send.at[ii, n], s_recv.at[ii, n], s).wait_recv()
        for n in range(16):
            for c in range(5):
                at = 96 * c if c < 4 else 384
                rest[n, 16 * c:16 * c + 16, 0:96] = rrest[ii, n, :, at:at + 96]

        def rows_of(plane):
            four = pl.ds(4 * plane, 4)
            return jnp.concatenate([rmain[ii, four].reshape(320, 128), rest[four].reshape(320, 128)], axis=1)

        for n0, n1 in ((0, 256), (256, 512), (512, 768), (768, 896)):
            t = dot(rows_of(0), mall[0, :, n0:n1])
            for b in range(1, 4):
                t += dot(rows_of(b), mall[b, :, n0:n1])
            mine = rows_of(a)
            t += dot(mine, mall[4, :, n0:n1]) + dot(mine, mall[5, :, n0:n1])
            for k, h in enumerate(split3(t)):
                tt[k, :, n0:n1] = h
        t0, t1, t2 = tt[0], tt[1], tt[2]
        same = dot_nt(t0, t0) + dot_nt(t1, t1)
        cross = dot_nt(t0, t1) + dot_nt(t0, t2)
        if ii == 0:
            ks[...] = same
            kx[...] = cross
        else:
            cross = kx[...] + cross
            ks[...] += same + cross + jnp.transpose(cross)

    t_and_k(0)
    for j in range(3):
        remote(fsend, frecv.at[planes[j]], f_send.at[j], f_recv.at[planes[j]], (planes[j], o)).wait_recv()
    weights = times_metric(lanes_of([frecv[b] for b in range(4)]))
    w_row = as_row(2.0 * weights)

    lane = lax.broadcasted_iota(jnp.int32, (8, 128), 1)
    w0, w1 = jnp.broadcast_to(w_row[:, :128], (8, 128)), jnp.broadcast_to(w_row[:, 128:224], (8, 96))

    zero32 = jnp.zeros((8, 32), F32)

    def coul(k, carry):
        for j in range(4):
            rows = pl.ds(pl.multiple_of(k * 32 + 8 * j, 8), 8)
            acc = jnp.zeros((8, 128), F32)
            for m in range(80):
                z = jnp.concatenate([bb[m, rows, 128:224] * w1, zero32], axis=1)
                col = jnp.sum(bb[m, rows, 0:128] * w0 + z, axis=1, keepdims=True)
                acc = jnp.where(lane == m, col, acc)
            jacc[rows, :] = acc[:, :80]
        return carry

    lax.fori_loop(0, 10, coul, 0)
    jt = jnp.transpose(jacc[...])

    t_and_k(1)

    def packed(x):
        tail = jnp.concatenate([x[56:, :48], jnp.concatenate([x[56:, 48:], jnp.zeros((24, 16), F32)], axis=1),
                                jnp.zeros((8, 48), F32)], axis=0)
        return jnp.concatenate([x[:56], tail], axis=1)

    for c in range(4):
        for k in range(4):
            gs[k % 2, k // 2, c] = packed(jnp.where(o == k, jt[:, 80 * c:80 * c + 80], 0.0)
                                          - ks[80 * k:80 * k + 80, 80 * c:80 * c + 80])
    far = 2 * (1 - a // 2)
    halves = [pl.ds(far, 2), pl.ds(2 - far, 2)]
    pairs = [remote(gs.at[1 - core, :, half], gp.at[:, half], p_sems.at[0, k], p_sems.at[1, k], (a, core_mate))
             for k, half in enumerate(halves)]
    for cp in pairs:
        cp.start()

    def r_copy(k):
        plane, y = planes[k // 2], (row_y + k % 2) % 2
        return remote(gf.at[y, plane], gr.at[a, row_y], r_send.at[k], r_recv.at[a, row_y], (plane, 2 * y + core))

    r_order = (0, 1, 2, 3, 4, 5, 7)
    for j, half in enumerate(halves):
        pairs[j].wait()
        gf[:, half] = gs[core, :, half] + gp[:, half]
        for k in r_order[4 * j:4 * j + 4]:
            r_copy(k).start()
    total = gf[row_y, a]
    for k in r_order:
        plane, y = planes[k // 2], (row_y + k % 2) % 2
        remote(gf.at[y, plane], gr.at[plane, y], r_send.at[k], r_recv.at[plane, y], (plane, 2 * y + core)).wait_recv()
        total = total + gr[plane, y]
    out_ref[0] = jnp.concatenate([total[:, :80], jnp.concatenate([total[0:24, 80:128], total[24:48, 80:112]], axis=1)], axis=0)


    for dest in peers:
        main_copy(0, dest, pl.ds(0, 80)).wait_send()
        main_copy(1, dest, pl.ds(0, 80)).wait_send()
        rest_copy(0, dest).wait_send()
        rest_copy(1, dest).wait_send()
        g_copy(dest).wait_send()
    for k in r_order:
        r_copy(k).wait_send()
    for r in range(3):
        relay(r, 'drain')
    for j in range(3):
        f_copy(j).wait_send()
        for k in range(3):
            mf_copy(planes[j], o, o, k).wait_send()


def solution(mesh):
    def local_fock(ints_blk, metric_blk, orbitals):
        dma = pltpu.SemaphoreType.DMA
        return pl.pallas_call(
            kernel,
            name='fock',
            out_shape=jax.ShapeDtypeStruct((1, 80, 80), F32),
            in_specs=[pl.BlockSpec(memory_space=pl.ANY), pl.BlockSpec(memory_space=pl.ANY),
                      pl.BlockSpec(memory_space=pltpu.VMEM)],
            out_specs=pl.BlockSpec(memory_space=pltpu.VMEM),
            scratch_shapes=[
                pltpu.VMEM((80, 320, 224), F32),
                pltpu.VMEM((2, 512, 128), F32),
                pltpu.VMEM((32, 80, 128), BF16),
                pltpu.VMEM((32, 16, 512), BF16),
                pltpu.VMEM((2, 16, 80, 128), BF16),
                pltpu.VMEM((2, 16, 16, 512), BF16),
                pltpu.VMEM((16, 80, 128), BF16),
                pltpu.VMEM((6, 256, 896), BF16),
                pltpu.VMEM((224, 896), F32),
                pltpu.VMEM((80, 32, 128), F32),
                pltpu.VMEM((96, 1024), BF16),
                pltpu.VMEM((3, 320, 896), BF16),
                pltpu.VMEM((320, 320), F32),
                pltpu.VMEM((320, 320), F32),
                pltpu.VMEM((320, 80), F32),
                pltpu.VMEM((32, 256), F32),
                pltpu.VMEM((1, 256), F32),
                pltpu.VMEM((16, 1, 256), F32),
                pltpu.VMEM((1, 256), F32),
                pltpu.VMEM((4, 1, 256), F32),
                pltpu.VMEM((2, 2, 4, 56, 128), F32),
                pltpu.VMEM((2, 4, 56, 128), F32),
                pltpu.VMEM((2, 4, 56, 128), F32),
                pltpu.VMEM((4, 2, 56, 128), F32),
                dma((20,)), dma(()),
                dma((4, 16)), dma((4, 16)),
                dma((4, 2)), dma((4,)),
                dma((4, 3)), dma((4, 4)),
                dma((16,)), dma((16,)),
                dma((3,)), dma((4,)),
                dma((2, 2)), dma((8,)), dma((4, 2)),
            ],
            compiler_params=pltpu.CompilerParams(collective_id=0, has_side_effects=True, vmem_limit_bytes=67043328),
        )(jnp.transpose(ints_blk, (1, 2, 0)), metric_blk, jnp.transpose(orbitals[0]))

    return jax.shard_map(local_fock, mesh=mesh, in_specs=(P(('sys', 'aux'), 'orb', None), P(('sys', 'aux'), None), P('sys', None, None)), out_specs=P('sys', 'orb', 'aux'), check_vma=False)
```
